32 devices in a mesh: slab: 8 (over y, x, core), chan: 4 (over z).
Axes of the slice: x: 2, y: 2, z: 4, core: 2. Of those that a mesh axis runs over, the one named last changes fastest.
Arguments:
- features: bfloat16 [96, 16384], P('chan', 'slab'), may hold values from -1 to 3
- coords: bfloat16 [3, 16384], P(None, 'slab'), may hold values from 0 to 1
- send_rows: int32 [2, 8192], P(None, 'slab'), may hold values from 0 to 2047
- send_count: int32 [2, 8], P(None, 'slab'), may hold values from 1 to 1024, as said below
- neighbours: int32 [1024, 128], P('slab'), may hold values from 0 to 4095, as said below
- neighbour_count: int32 [1024], P('slab'), may hold values from 32 to 128
- geom_weight: bfloat16 [80, 6], replicated, may hold values from -3.5 to 3.5
- feat_weight: bfloat16 [80, 96], replicated, may hold values from -0.625 to 0.625
- bias_one: float32 [80], replicated, may hold values from -3 to 3
- hidden_weight: bfloat16 [80, 80], replicated, may hold values from -1 to 1
- bias_two: float32 [80], replicated, may hold values from -3 to 3
- out_weight: bfloat16 [96, 80], replicated, may hold values from -1 to 1
- bias_three: float32 [96], replicated, may hold values from -3 to 3
Outputs:
- latent: float32 [96, 1024], P('chan', 'slab')
The draws below stay inside these ranges and needn't reach their ends.
Inputs may be any that keep to these rules, and one draw needn't show every extreme that they name: `send_count`: every slab has at least one live slot in each direction; some slab has all 1024 slots of its lower list live. `neighbours`: entries index the slab's point table: below 2048 own points, then 1024 slots from the slab below, then 1024 from the slab above; slot 0 of every node is an own point; nodes of the lower plane of a slab use the slots from below, those of the upper plane the slots from above, and may name dead slots.
All inputs are finite; a program needn't handle non-finite values.
Results may differ from the reference program's by a relative error of at most 0.0013.
Values may be sent and summed in bfloat16 or wider, within the bound.
No kernel may reach another device: no remote copies, remote signals or barrier semaphores. Data moves between devices by JAX's collectives and lax.ppermute only.
A program may use at most 64 MiB of HBM per device.

```python
import jax
import jax.numpy as jnp
from jax import lax

F = 96
KH = 80
K = 128
ZD = 2
GX = 16
GY = 4
PTS_DEV = 2048
SEND = 1024
POINTS = 16384
NODES = 1024
N_SLAB = 8


def draw_send_count(key, part):
    counts = jax.random.randint(jax.random.fold_in(key, 7), (2, N_SLAB), 1, SEND + 1)
    return counts.at[0, 0].set(SEND).astype(jnp.int32)


def draw_neighbours(key, part):
    keys = jax.random.split(jax.random.fold_in(key, 11), 3)
    local = jax.random.randint(keys[0], (NODES, K), 0, PTS_DEV)
    slot = jax.random.randint(keys[1], (NODES, K), 0, SEND)
    kind = jax.random.randint(keys[2], (NODES, K), 0, 10)
    plane = jnp.arange(NODES, dtype=jnp.int32) // (GX * GY) % ZD
    side = jnp.where(plane < ZD // 2, PTS_DEV, PTS_DEV + SEND)
    picked = jnp.where(kind < 4, side[:, None] + slot, local)
    picked = picked.at[:, 0].set(local[:, 0])
    return picked.astype(jnp.int32)


def set_ends(values, rng, low, top_value):
    longest = values.shape.index(max(values.shape))
    spots = []
    for shift in (0, 1):
        where = [jax.random.randint(jax.random.fold_in(rng, axis), (), 0, length) for axis, length in enumerate(values.shape)]
        where[longest] = (where[longest] + shift) % values.shape[longest]
        spots.append(tuple(where))
    return values.at[spots[0]].set(low).at[spots[1]].set(top_value)


def steps_of(rng, extent, pieces, smallest, high):
    level, own = 1.0, jax.random.fold_in(rng, 6)
    for position, blocks in pieces:
        draws = jnp.exp(jax.random.uniform(jax.random.fold_in(own, position), (blocks,), jnp.float32, smallest / len(pieces), high / len(pieces)))
        level = level * jnp.repeat(draws, extent[position] // blocks).reshape([-1 if axis == position else 1 for axis in range(len(extent))])
    return level


def scatter_about(own_key, extent, scale, most, held_as=jnp.bfloat16):
    entries = jax.random.normal(own_key, extent, jnp.float32) * scale
    return jnp.minimum(jnp.maximum(entries, -most), most).astype(held_as)


def setup_inputs(seed: int = 0) -> dict:
    seeds = jax.random.split(jax.random.key(seed), 14)
    return {
        "features": jnp.clip(-1.0 + 4.0 * jax.random.uniform(seeds[0], (F, POINTS), jnp.float32) ** steps_of(seeds[0], (F, POINTS), ((0, 4), (1, 8)), -0.2, 0.2), -1.0, 3.0).astype(jnp.bfloat16),
        "coords": jnp.clip(1.0 * jax.random.uniform(seeds[1], (3, POINTS), jnp.float32) ** steps_of(seeds[1], (3, POINTS), ((1, 8),), -0.2, 0.2), 0.0, 1.0).astype(jnp.bfloat16),
        "send_rows": set_ends(jax.random.randint(seeds[2], (2, SEND * N_SLAB), 0, PTS_DEV), jax.random.fold_in(seeds[2], 1), 0, PTS_DEV - 1).astype(jnp.int32),
        "send_count": draw_send_count(jax.random.fold_in(seeds[13], 71), 0),
        "neighbours": draw_neighbours(jax.random.fold_in(seeds[13], 71), 0),
        "neighbour_count": set_ends(jax.random.randint(seeds[5], (NODES,), K // 4, K + 1), jax.random.fold_in(seeds[5], 1), K // 4, K).astype(jnp.int32),
        "geom_weight": scatter_about(seeds[6], (KH, 6), 3 ** -0.5, 3.5),
        "feat_weight": scatter_about(seeds[7], (KH, F), F ** -0.5, 0.625),
        "bias_one": scatter_about(seeds[8], (KH,), 0.5, 3.0, jnp.float32),
        "hidden_weight": scatter_about(seeds[9], (KH, KH), (KH // 2) ** -0.5, 1.0),
        "bias_two": scatter_about(seeds[10], (KH,), 0.5, 3.0, jnp.float32),
        "out_weight": scatter_about(seeds[11], (F, KH), (KH // 2) ** -0.5, 1.0),
        "bias_three": scatter_about(seeds[12], (F,), 0.5, 3.0, jnp.float32),
    }


def node_term(geom_weight, bias_one, node_ids, depth):
    along_x = ((node_ids % GX).astype(jnp.float32) + 0.5) / GX
    along_y = (((node_ids // GX) % GY).astype(jnp.float32) + 0.5) / GY
    along_z = ((node_ids // (GX * GY)).astype(jnp.float32) + 0.5) / depth
    geom = geom_weight[:, 0:3].astype(jnp.float32)
    return (geom[:, 0:1] * along_x[None, :] + geom[:, 1:2] * along_y[None, :]
            + geom[:, 2:3] * along_z[None, :] + bias_one[:, None])


def kernel_block(pre_table, value_table, flag_table, nbr, counts, node_pre, hidden_weight, bias_two, out_rows, bias_rows):
    nodes, slots = nbr.shape
    hidden = pre_table.shape[0]
    flat = nbr.reshape(-1)
    gathered = jnp.take(pre_table, flat, axis=1).astype(jnp.float32).reshape(hidden, nodes, slots)
    first = jax.nn.gelu(gathered + node_pre[:, :, None]).reshape(hidden, nodes * slots).astype(jnp.bfloat16)
    second = jax.nn.gelu(jnp.dot(hidden_weight, first, preferred_element_type=jnp.float32) + bias_two[:, None]).astype(jnp.bfloat16)
    kappa = jnp.dot(out_rows, second, preferred_element_type=jnp.float32) + bias_rows[:, None]
    values = jnp.take(value_table, flat, axis=1).astype(jnp.float32)
    used = (jnp.arange(slots, dtype=jnp.int32)[None, :] < counts[:, None]).astype(jnp.float32)
    flags = jnp.take(flag_table, flat).astype(jnp.float32) * used.reshape(-1)
    total = (kappa * values * flags[None, :]).reshape(out_rows.shape[0], nodes, slots).sum(axis=2)
    weight = flags.reshape(nodes, slots).sum(axis=1)
    return total / weight[None, :]


def encode(pre_table, value_table, flag_table, nbr, counts, first_id, depth, geom_weight, bias_one, hidden_weight, bias_two, out_rows, bias_rows):
    nodes = nbr.shape[0]
    block = min(128, nodes)
    blocks = nodes // block

    def one_block(index):
        start = index * block
        ids = first_id + start + jnp.arange(block, dtype=jnp.int32)
        node_pre = node_term(geom_weight, bias_one, ids, depth)
        part_nbr = lax.dynamic_slice_in_dim(nbr, start, block, 0)
        part_cnt = lax.dynamic_slice_in_dim(counts, start, block, 0)
        return kernel_block(pre_table, value_table, flag_table, part_nbr, part_cnt, node_pre, hidden_weight, bias_two, out_rows, bias_rows)

    result = lax.map(one_block, jnp.arange(blocks, dtype=jnp.int32))
    return result.transpose(1, 0, 2).reshape(out_rows.shape[0], nodes)


def reference(features, coords, send_rows, send_count, neighbours, neighbour_count, geom_weight, feat_weight, bias_one, hidden_weight, bias_two, out_weight, bias_three):
    slabs = N_SLAB
    pts = PTS_DEV
    send = SEND
    pre = (jnp.dot(feat_weight, features, preferred_element_type=jnp.float32)
           + jnp.dot(geom_weight[:, 3:6], coords, preferred_element_type=jnp.float32)).astype(jnp.bfloat16)
    offsets = (jnp.arange(slabs, dtype=jnp.int32) * pts)[None, :, None]
    rows = (send_rows.reshape(2, slabs, send) + offsets).reshape(-1)
    live = (jnp.arange(send, dtype=jnp.int32)[None, None, :] < send_count[:, :, None]).astype(jnp.bfloat16)
    pre_send = jnp.take(pre, rows, axis=1).reshape(KH, 2, slabs, send) * live[None]
    feat_send = jnp.take(features, rows, axis=1).reshape(F, 2, slabs, send) * live[None]

    def from_below(x):
        return jnp.concatenate([jnp.zeros_like(x[..., :1, :]), x[..., :-1, :]], axis=-2)

    def from_above(x):
        return jnp.concatenate([x[..., 1:, :], jnp.zeros_like(x[..., :1, :])], axis=-2)

    pre_tables = jnp.concatenate([pre.reshape(KH, slabs, pts), from_below(pre_send[:, 1]), from_above(pre_send[:, 0])], axis=2)
    value_tables = jnp.concatenate([features.reshape(F, slabs, pts), from_below(feat_send[:, 1]), from_above(feat_send[:, 0])], axis=2)
    flag_tables = jnp.concatenate([jnp.ones((slabs, pts), jnp.bfloat16), from_below(live[1]), from_above(live[0])], axis=1)
    per_slab = ZD * GY * GX
    nbr = neighbours.reshape(slabs, per_slab, K)
    cnt = neighbour_count.reshape(slabs, per_slab)
    depth = ZD * slabs

    def one_slab(index):
        return encode(pre_tables[:, index], value_tables[:, index], flag_tables[index], nbr[index], cnt[index],
                      index * per_slab, depth, geom_weight, bias_one, hidden_weight, bias_two, out_weight, bias_three)

    outs = lax.map(one_slab, jnp.arange(slabs, dtype=jnp.int32))
    return outs.transpose(1, 0, 2).reshape(F, slabs * per_slab)
```

```python
import jax
import jax.numpy as jnp
from jax import lax
from jax.experimental import pallas as pl
from jax.experimental.pallas import tpu as pltpu
from jax.sharding import PartitionSpec as P

ZD = 2
GX = 16
GY = 4
LANES = 128


def node_term(geom, bias, ids, depth):
    along_x = ((ids % GX).astype(jnp.float32) + 0.5) / GX
    along_y = ((ids // GX % GY).astype(jnp.float32) + 0.5) / GY
    along_z = ((ids // (GX * GY)).astype(jnp.float32) + 0.5) / depth
    return geom[0:1] * along_x + geom[1:2] * along_y + geom[2:3] * along_z + bias


def select_points(blocks, coords, send_rows, send_count, place):
    groups = len(blocks)
    chans, points = blocks[0].shape
    width = LANES // groups
    send = send_rows.shape[1]
    unroll = 16

    def kernel(*refs):
        block_refs = refs[:groups]
        coords_ref, rows_ref, count_ref, place_ref = refs[groups : groups + 4]
        own_ref, sent_ref, stack, table, picked = refs[groups + 4 :]
        member = place_ref[0]
        side = place_ref[1]
        for step in range(groups):
            base = pl.multiple_of((member ^ step) * width, width)
            empty = jnp.zeros((width - chans, points), jnp.bfloat16)
            stack[pl.ds(base, width), :] = jnp.concatenate([block_refs[step][...], empty], axis=0)
        stack[chans : chans + 3, :] = coords_ref[...]
        stack[chans + 3 : chans + 4, :] = jnp.ones((1, points), jnp.bfloat16)
        own = stack[...].T
        own_ref[...] = own
        table[...] = own.astype(jnp.float32)

        def gather(step, carry):
            base = step * unroll
            rows = [table[pl.ds(rows_ref[side, base + j], 1), :] for j in range(unroll)]
            for j in range(unroll):
                picked[pl.ds(base + j, 1), :] = rows[j]
            return carry

        lax.fori_loop(0, send // unroll, gather, 0)
        slot = lax.broadcasted_iota(jnp.int32, (send, LANES), 0)
        sent_ref[...] = jnp.where(slot < count_ref[side, 0], picked[...], 0.0).astype(jnp.bfloat16)

    smem = pl.BlockSpec(memory_space=pltpu.SMEM)
    vmem = pl.BlockSpec(memory_space=pltpu.VMEM)
    return pl.pallas_call(
        kernel,
        out_shape=(
            jax.ShapeDtypeStruct((points, LANES), jnp.bfloat16),
            jax.ShapeDtypeStruct((send, LANES), jnp.bfloat16),
        ),
        in_specs=[vmem] * (groups + 1) + [smem] * 3,
        out_specs=(vmem, vmem),
        scratch_shapes=[
            pltpu.VMEM((LANES, points), jnp.bfloat16),
            pltpu.VMEM((points, LANES), jnp.float32),
            pltpu.VMEM((send, LANES), jnp.float32),
        ],
        name="select_points",
    )(*blocks, coords, send_rows, send_count, place)


def encode(own, other, rows, place, table_weight, hidden_weight, out_weight, vectors, groups, chans, per_slab, depth):
    points = own.shape[0]
    send = other.shape[0]
    nodes, slots = rows.shape
    total_rows = points + send
    width = LANES // groups
    unroll = 16
    group_nodes = 8
    pairs = group_nodes * slots

    def kernel(own_ref, other_ref, rows_ref, place_ref, table_w, hidden_w, out_w, vec_ref, *rest):
        outs = rest[:groups]
        table, picked, acc, turned = rest[groups:]
        member = place_ref[0]
        first_id = place_ref[2]

        def fill(source, start, count):
            step = 256
            for at in range(0, count, step):
                both = jnp.dot(source[pl.ds(at, step), :], table_w[...], preferred_element_type=jnp.float32)
                pre = both[:, :LANES].astype(jnp.bfloat16).astype(jnp.float32)
                table[pl.ds(2 * (start + at), step, stride=2), :] = pre
                table[pl.ds(2 * (start + at) + 1, step, stride=2), :] = both[:, LANES:]

        fill(own_ref, 0, points)
        fill(other_ref, points, send)
        table[pl.ds(2 * total_rows, 8), :] = jnp.zeros((8, LANES), jnp.float32)

        acc[...] = jnp.zeros((LANES, LANES), jnp.float32)
        vec = vec_ref[...]
        bias_two = vec[4:5]
        bias_three = vec[5:6]

        def one_group(index, carry):
            start = index * group_nodes

            def gather(step, inner):
                node = step // (slots // unroll)
                slot = (step % (slots // unroll)) * unroll
                got = [
                    table[pl.ds(rows_ref[start + node, slot + j], 2), :] for j in range(unroll)
                ]
                for j in range(unroll):
                    picked[pl.ds(2 * (step * unroll + j), 2), :] = got[j]
                return inner

            lax.fori_loop(0, pairs // unroll, gather, 0)
            ids = first_id + start + lax.broadcasted_iota(jnp.int32, (group_nodes, 1), 0)
            node_pre = node_term(vec[0:3], vec[3:4], ids, depth)
            for node in range(group_nodes):
                pre = picked[pl.ds(2 * node * slots, slots, stride=2), :]
                val = picked[pl.ds(2 * node * slots + 1, slots, stride=2), :]
                first = jax.nn.gelu(pre + node_pre[node : node + 1]).astype(jnp.bfloat16)
                second = jnp.dot(first, hidden_w[...], preferred_element_type=jnp.float32)
                second = jax.nn.gelu(second + bias_two).astype(jnp.bfloat16)
                kappa = jnp.dot(second, out_w[...], preferred_element_type=jnp.float32) + bias_three
                total = jnp.sum(kappa * val, axis=0, keepdims=True)
                acc[pl.ds(member * nodes + start + node, 1), :] = total
            return carry

        lax.fori_loop(0, nodes // group_nodes, one_group, 0)
        flag_lane = chans + 3
        sums = acc[...]
        weight = sums[:, flag_lane : flag_lane + 1]
        here = lax.broadcasted_iota(jnp.int32, (LANES, 1), 0)
        mine = (here >= member * nodes) & (here < (member + 1) * nodes)
        scaled = sums / jnp.where(mine, weight, 1.0)
        turned[...] = scaled.T
        for step in range(groups):
            base = pl.multiple_of((member ^ step) * width, width)
            outs[step][...] = turned[pl.ds(base, chans), :]

    smem = pl.BlockSpec(memory_space=pltpu.SMEM)
    vmem = pl.BlockSpec(memory_space=pltpu.VMEM)
    return pl.pallas_call(
        kernel,
        out_shape=tuple(jax.ShapeDtypeStruct((chans, per_slab), jnp.float32) for _ in range(groups)),
        in_specs=[vmem, vmem, smem, smem] + [vmem] * 4,
        out_specs=(vmem,) * groups,
        scratch_shapes=[
            pltpu.VMEM((2 * total_rows + 8, LANES), jnp.float32),
            pltpu.VMEM((2 * pairs, LANES), jnp.float32),
            pltpu.VMEM((LANES, LANES), jnp.float32),
            pltpu.VMEM((LANES, LANES), jnp.float32),
        ],
        name="encode",
    )(own, other, rows, place, table_weight, hidden_weight, out_weight, vectors)


def shards(
    features,
    coords,
    send_rows,
    send_count,
    neighbours,
    neighbour_count,
    geom_weight,
    feat_weight,
    bias_one,
    hidden_weight,
    bias_two,
    out_weight,
    bias_three,
):
    groups = lax.axis_size("chan")
    slabs = lax.axis_size("slab")
    member = lax.axis_index("chan")
    slab_id = lax.axis_index("slab")
    depth = ZD * slabs
    chans, points = features.shape
    send = send_rows.shape[1]
    per_slab, slots = neighbours.shape
    hidden = hidden_weight.shape[0]
    share = per_slab // groups
    width = LANES // groups
    half = groups // ZD

    blocks = [features]
    for step in range(1, groups):
        blocks.append(lax.ppermute(features, "chan", [(i, i ^ step) for i in range(groups)]))

    upper = (member < half).astype(jnp.int32)
    first_id = slab_id * per_slab + member * share
    place = jnp.stack([member, upper, first_id]).astype(jnp.int32)
    own, sent = select_points(blocks, coords, send_rows, send_count, place)
    pairs = []
    for slab in range(slabs):
        for who in range(groups):
            target = slab + 1 if who < half else slab - 1
            if 0 <= target < slabs:
                pairs.append((slab * groups + who, target * groups + who))
    other = lax.ppermute(sent, ("slab", "chan"), pairs)

    part_nbr = lax.dynamic_slice_in_dim(neighbours, member * share, share, 0)
    part_cnt = lax.dynamic_slice_in_dim(neighbour_count, member * share, share, 0)
    row = jnp.where(part_nbr >= points + send, part_nbr - send, part_nbr)
    slot = lax.broadcasted_iota(jnp.int32, (share, slots), 1)
    rows = 2 * jnp.where(slot < part_cnt[:, None], row, points + send)

    def lanes_of(weight):
        lead = weight.shape[:-1]
        split = weight.reshape(lead + (groups, chans))
        return jnp.pad(split, [(0, 0)] * len(lead) + [(0, 0), (0, width - chans)]).reshape(lead + (LANES,))

    feat_rows = lanes_of(feat_weight)
    spot = jnp.arange(LANES)
    geom = jnp.pad(geom_weight[:, 3:6], ((0, 0), (chans, LANES - chans - 3)))
    pre_weight = jnp.pad((feat_rows + geom).T, ((0, 0), (0, LANES - hidden)))
    table_weight = jnp.concatenate([pre_weight, jnp.eye(LANES, dtype=jnp.bfloat16)], axis=1)
    hidden_t = jnp.pad(hidden_weight.T, ((0, LANES - hidden), (0, LANES - hidden)))
    out_t = jnp.pad(lanes_of(out_weight.T), ((0, LANES - hidden), (0, 0)))
    tail = (0, LANES - hidden)
    vectors = jnp.concatenate(
        [
            jnp.pad(geom_weight[:, 0:3].astype(jnp.float32).T, ((0, 0), tail)),
            jnp.pad(bias_one, tail)[None],
            jnp.pad(bias_two, tail)[None],
            (lanes_of(bias_three) + (spot == chans + 3))[None],
            jnp.zeros((2, LANES), jnp.float32),
        ],
        axis=0,
    )
    pieces = encode(
        own, other, rows, place, table_weight, hidden_t, out_t, vectors, groups, chans, per_slab, depth
    )
    result = pieces[0]
    for step in range(1, groups):
        result = result + lax.ppermute(pieces[step], "chan", [(i, i ^ step) for i in range(groups)])
    return result


def solution(mesh):
    placed = (
        P("chan", "slab"),
        P(None, "slab"),
        P(None, "slab"),
        P(None, "slab"),
        P("slab", None),
        P("slab"),
        P(),
        P(),
        P(),
        P(),
        P(),
        P(),
        P(),
    )
    return jax.shard_map(
        shards, mesh=mesh, in_specs=placed, out_specs=P("chan", "slab"), check_vma=False
    )
```

```python
import jax
import jax.numpy as jnp
from jax import lax
from jax.experimental import pallas as pl
from jax.experimental.pallas import tpu as pltpu
from jax.sharding import PartitionSpec as P

ZD = 2
GX = 16
GY = 4
LANES = 128
CHUNK = 16
BLOCK = 64

SMEM = pl.BlockSpec(memory_space=pltpu.SMEM)
VMEM = pl.BlockSpec(memory_space=pltpu.VMEM)
ANY = pl.BlockSpec(memory_space=pl.ANY)


def node_term(geom, bias, ids, depth):
    along_x = ((ids % GX).astype(jnp.float32) + 0.5) / GX
    along_y = ((ids // GX % GY).astype(jnp.float32) + 0.5) / GY
    along_z = ((ids // (GX * GY)).astype(jnp.float32) + 0.5) / depth
    return geom[0:1] * along_x + geom[1:2] * along_y + geom[2:3] * along_z + bias


def plan_pairs(neighbours, neighbour_count, place, nodes, points, send):
    slots = neighbours.shape[1]
    per_node = slots // CHUNK
    most = nodes * per_node
    nothing = 2 * (points + send)

    def kernel(nbr_ref, count_ref, place_ref, rows_ref, list_ref, total_ref):
        start = place_ref[3]
        lane = lax.broadcasted_iota(jnp.int32, (1, slots), 1)

        def one_node(node, at):
            count = count_ref[start + node]
            row = nbr_ref[pl.ds(start + node, 1), :]
            row = jnp.where(row >= points + send, row - send, row)
            rows_ref[pl.ds(node, 1), :] = jnp.where(lane < count, 2 * row, nothing)
            for piece in range(per_node):
                list_ref[at + piece] = node * per_node + piece
            return at + (count + CHUNK - 1) // CHUNK

        used = lax.fori_loop(0, nodes, one_node, 0)
        rows_ref[pl.ds(nodes, 8), :] = jnp.full((8, slots), nothing, jnp.int32)
        total_ref[0] = (used + BLOCK - 1) // BLOCK

        def fill(step, carry):
            list_ref[used + step] = most
            return carry

        lax.fori_loop(0, BLOCK, fill, 0)

    return pl.pallas_call(
        kernel,
        out_shape=(
            jax.ShapeDtypeStruct((nodes + 8, slots), jnp.int32),
            jax.ShapeDtypeStruct((most + BLOCK,), jnp.int32),
            jax.ShapeDtypeStruct((1,), jnp.int32),
        ),
        in_specs=[VMEM, SMEM, SMEM],
        out_specs=(VMEM, SMEM, SMEM),
        name="plan_pairs",
    )(neighbours, neighbour_count, place)


def select_points(blocks, coords, send_rows, send_count, place, after):
    groups = len(blocks)
    chans, points = blocks[0].shape
    width = LANES // groups
    send = send_rows.shape[0] // 2
    unroll = 32

    def kernel(*refs):
        block_refs = refs[:groups]
        coords_ref, rows_ref, count_ref, place_ref = refs[groups : groups + 4]
        own_ref, sent_ref, stack, table, picked = refs[groups + 4 + len(after) :]
        member = place_ref[0]
        side = place_ref[1]
        for step in range(groups):
            base = pl.multiple_of((member ^ step) * width, width)
            empty = jnp.zeros((width - chans, points), jnp.bfloat16)
            stack[pl.ds(base, width), :] = jnp.concatenate([block_refs[step][...], empty], axis=0)
        stack[chans : chans + 3, :] = coords_ref[...]
        stack[chans + 3 : chans + 4, :] = jnp.ones((1, points), jnp.bfloat16)
        own = stack[...].T
        own_ref[...] = own
        table[...] = own.astype(jnp.float32)

        def gather(step, carry):
            base = step * unroll
            first = side * send + base
            rows = [table[pl.ds(rows_ref[first + j], 1), :] for j in range(unroll)]
            for j in range(unroll):
                picked[pl.ds(base + j, 1), :] = rows[j]
            return carry

        lax.fori_loop(0, send // unroll, gather, 0)
        slot = lax.broadcasted_iota(jnp.int32, (send, LANES), 0)
        sent_ref[...] = jnp.where(slot < count_ref[side, 0], picked[...], 0.0).astype(jnp.bfloat16)

    return pl.pallas_call(
        kernel,
        out_shape=(
            jax.ShapeDtypeStruct((points, LANES), jnp.bfloat16),
            jax.ShapeDtypeStruct((send, LANES), jnp.bfloat16),
        ),
        in_specs=[VMEM] * (groups + 1) + [SMEM] * 3 + [ANY] * len(after),
        out_specs=(VMEM, VMEM),
        scratch_shapes=[
            pltpu.VMEM((LANES, points), jnp.bfloat16),
            pltpu.VMEM((points, LANES), jnp.float32),
            pltpu.VMEM((send, LANES), jnp.float32),
        ],
        name="select_points",
    )(*blocks, coords, send_rows, send_count, place, *after)


def encode(own, other, plan, place, weights, chans, width, depth):
    rows, chunks, total = plan
    table_weight, hidden_weight, out_weight, vectors = weights
    points = own.shape[0]
    send = other.shape[0]
    nodes = rows.shape[0] - 8
    slots = rows.shape[1]
    shift = (slots // CHUNK).bit_length() - 1
    total_rows = points + send
    pairs = BLOCK * CHUNK
    all_nodes = ZD * nodes

    def kernel(
        own_ref, other_ref, rows_ref, list_ref, total_ref, place_ref, table_w, hidden_w, out_w,
        vec_ref, keep_ref, give_ref, table, picked, node_pre, acc, turned,
    ):
        parity = place_ref[1]
        first_id = place_ref[2]

        def fill(source, start, count):
            step = 256
            for at in range(0, count, step):
                both = jnp.dot(source[pl.ds(at, step), :], table_w[...], preferred_element_type=jnp.float32)
                pre = both[:, :LANES].astype(jnp.bfloat16).astype(jnp.float32)
                table[pl.ds(2 * (start + at), step, stride=2), :] = pre
                table[pl.ds(2 * (start + at) + 1, step, stride=2), :] = both[:, LANES:]

        fill(own_ref, 0, points)
        fill(other_ref, points, send)
        table[pl.ds(2 * total_rows, 8), :] = jnp.zeros((8, LANES), jnp.float32)

        vec = vec_ref[...]
        bias_two = vec[4:5]
        bias_three = vec[5:6]
        ids = first_id + lax.broadcasted_iota(jnp.int32, (nodes + 8, 1), 0)
        node_pre[...] = node_term(vec[0:3], vec[3:4], ids, depth)
        acc[...] = jnp.zeros((nodes + 8, LANES), jnp.float32)

        def one_block(index, carry):
            names = [list_ref[index * BLOCK + piece] for piece in range(BLOCK)]
            for piece in range(BLOCK):
                at = names[piece] * CHUNK
                got = [table[pl.ds(rows_ref[at + j], 2), :] for j in range(CHUNK)]
                for j in range(CHUNK):
                    picked[pl.ds(2 * (piece * CHUNK + j), 2), :] = got[j]
            step = 8
            for group in range(BLOCK // step):
                base = group * step * CHUNK
                offset = jnp.concatenate(
                    [
                        jnp.broadcast_to(
                            node_pre[pl.ds(names[group * step + i] >> shift, 1), :], (CHUNK, LANES)
                        )
                        for i in range(step)
                    ],
                    axis=0,
                )
                pre = picked[pl.ds(2 * base, step * CHUNK, stride=2), :]
                val = picked[pl.ds(2 * base + 1, step * CHUNK, stride=2), :]
                first = jax.nn.gelu(pre + offset).astype(jnp.bfloat16)
                second = jnp.dot(first, hidden_w[...], preferred_element_type=jnp.float32)
                second = jax.nn.gelu(second + bias_two).astype(jnp.bfloat16)
                kappa = jnp.dot(second, out_w[...], preferred_element_type=jnp.float32) + bias_three
                product = kappa * val
                for i in range(step):
                    part = jnp.sum(product[i * CHUNK : (i + 1) * CHUNK], axis=0, keepdims=True)
                    spot = pl.ds(names[group * step + i] >> shift, 1)
                    acc[spot, :] = acc[spot, :] + part
            return carry

        lax.fori_loop(0, total_ref[0], one_block, 0)
        sums = acc[0:nodes]
        means = (sums / sums[:, LANES - 1 :]).T
        blank = jnp.zeros((LANES, nodes), jnp.float32)
        low = jnp.where(parity == 1, means, blank)
        turned[...] = jnp.concatenate([low, means - low], axis=1)
        mine = pl.multiple_of((1 - parity) * width, width)
        theirs = pl.multiple_of(parity * width, width)
        keep_ref[...] = turned[pl.ds(mine, chans), :]
        give_ref[...] = turned[pl.ds(theirs, chans), :]

    piece = jax.ShapeDtypeStruct((chans, all_nodes), jnp.float32)
    return pl.pallas_call(
        kernel,
        out_shape=(piece, piece),
        in_specs=[VMEM, VMEM] + [SMEM] * 4 + [VMEM] * 4,
        out_specs=(VMEM, VMEM),
        scratch_shapes=[
            pltpu.VMEM((2 * total_rows + 8, LANES), jnp.float32),
            pltpu.VMEM((2 * pairs, LANES), jnp.float32),
            pltpu.VMEM((nodes + 8, LANES), jnp.float32),
            pltpu.VMEM((nodes + 8, LANES), jnp.float32),
            pltpu.VMEM((LANES, all_nodes), jnp.float32),
        ],
        name="encode",
    )(
        own, other, rows.reshape(-1), chunks, total, place, table_weight, hidden_weight, out_weight,
        vectors,
    )


def shards(
    features,
    coords,
    send_rows,
    send_count,
    neighbours,
    neighbour_count,
    geom_weight,
    feat_weight,
    bias_one,
    hidden_weight,
    bias_two,
    out_weight,
    bias_three,
):
    groups = lax.axis_size("chan")
    slabs = lax.axis_size("slab")
    member = lax.axis_index("chan")
    slab_id = lax.axis_index("slab")
    depth = ZD * slabs
    chans, points = features.shape
    send = send_rows.shape[1]
    per_slab = neighbours.shape[0]
    hidden = hidden_weight.shape[0]
    nodes = per_slab // ZD
    width = LANES // groups

    blocks = [features]
    for step in range(1, groups):
        blocks.append(lax.ppermute(features, "chan", [(i, i ^ step) for i in range(groups)]))

    plane = member % 2
    start = plane * nodes
    upper = 1 - plane
    place = jnp.stack([member, upper, slab_id * per_slab + start, start]).astype(jnp.int32)
    plan = plan_pairs(neighbours, neighbour_count, place, nodes, points, send)

    def lanes_of(weight):
        lead = weight.shape[:-1]
        split = weight.reshape(lead + (groups, chans))
        return jnp.pad(split, [(0, 0)] * len(lead) + [(0, 0), (0, width - chans)]).reshape(lead + (LANES,))

    first_lane = (member // 2) * 2 * width

    def pair_of(weight):
        part = lax.dynamic_slice_in_dim(lanes_of(weight), first_lane, 2 * width, weight.ndim - 1)
        return jnp.pad(part, [(0, 0)] * (weight.ndim - 1) + [(0, LANES - 2 * width)])

    row = jnp.arange(LANES)[:, None]
    lane = jnp.arange(LANES)[None, :]
    take = ((row == first_lane + lane) & (lane < 2 * width)) | ((row == chans + 3) & (lane == LANES - 1))
    geom = jnp.pad(geom_weight[:, 3:6], ((0, 0), (chans, LANES - chans - 3)))
    pre_weight = jnp.pad((lanes_of(feat_weight) + geom).T, ((0, 0), (0, LANES - hidden)))
    table_weight = jnp.concatenate([pre_weight, take.astype(jnp.bfloat16)], axis=1)
    hidden_t = jnp.pad(hidden_weight.T, ((0, LANES - hidden), (0, LANES - hidden)))
    out_t = jnp.pad(pair_of(out_weight.T), ((0, LANES - hidden), (0, 0)))
    tail = (0, LANES - hidden)
    vectors = jnp.concatenate(
        [
            jnp.pad(geom_weight[:, 0:3].astype(jnp.float32).T, ((0, 0), tail)),
            jnp.pad(bias_one, tail)[None],
            jnp.pad(bias_two, tail)[None],
            pair_of(bias_three)[None] + (lane == LANES - 1),
            jnp.zeros((2, LANES), jnp.float32),
        ],
        axis=0,
    )
    weights = (table_weight, hidden_t, out_t, vectors)

    own, sent = select_points(
        blocks, coords, send_rows.reshape(-1), send_count, place, plan + weights
    )
    moves = []
    for slab in range(slabs):
        for who in range(groups):
            target = slab + 1 if who % 2 == 0 else slab - 1
            if 0 <= target < slabs:
                moves.append((slab * groups + who, target * groups + who))
    other = lax.ppermute(sent, ("slab", "chan"), moves)
    keep, give = encode(own, other, plan, place, weights, chans, width, depth)
    return keep + lax.ppermute(give, "chan", [(i, i ^ 1) for i in range(groups)])


def solution(mesh):
    placed = (
        P("chan", "slab"),
        P(None, "slab"),
        P(None, "slab"),
        P(None, "slab"),
        P("slab", None),
        P("slab"),
        P(),
        P(),
        P(),
        P(),
        P(),
        P(),
        P(),
    )
    return jax.shard_map(
        shards, mesh=mesh, in_specs=placed, out_specs=P("chan", "slab"), check_vma=False
    )
```

```python
import jax
import jax.numpy as jnp
from jax import lax
from jax.experimental import pallas as pl
from jax.experimental.pallas import tpu as pltpu
from jax.sharding import PartitionSpec as P

ZD = 2
GX = 16
GY = 4
LANES = 128
CHUNK = 16
BLOCK = 64

SMEM = pl.BlockSpec(memory_space=pltpu.SMEM)
VMEM = pl.BlockSpec(memory_space=pltpu.VMEM)
ANY = pl.BlockSpec(memory_space=pl.ANY)


def node_term(geom, bias, ids, depth):
    along_x = ((ids % GX).astype(jnp.float32) + 0.5) / GX
    along_y = ((ids // GX % GY).astype(jnp.float32) + 0.5) / GY
    along_z = ((ids // (GX * GY)).astype(jnp.float32) + 0.5) / depth
    return geom[0:1] * along_x + geom[1:2] * along_y + geom[2:3] * along_z + bias


def plan_pairs(neighbours, neighbour_count, place, nodes, points, send):
    slots = neighbours.shape[1]
    per_node = slots // CHUNK
    most = nodes * per_node
    nothing = 2 * (points + send)

    def kernel(nbr_ref, count_ref, place_ref, rows_ref, list_ref, total_ref):
        start = place_ref[3]
        lane = lax.broadcasted_iota(jnp.int32, (1, slots), 1)

        def one_node(node, at):
            count = count_ref[start + node]
            row = nbr_ref[pl.ds(start + node, 1), :]
            row = jnp.where(row >= points + send, row - send, row)
            rows_ref[pl.ds(node, 1), :] = jnp.where(lane < count, 2 * row, nothing)
            for piece in range(per_node):
                list_ref[at + piece] = node * per_node + piece
            return at + (count + CHUNK - 1) // CHUNK

        used = lax.fori_loop(0, nodes, one_node, 0)
        rows_ref[pl.ds(nodes, 8), :] = jnp.full((8, slots), nothing, jnp.int32)
        total_ref[0] = (used + BLOCK - 1) // BLOCK

        def fill(step, carry):
            list_ref[used + step] = most
            return carry

        lax.fori_loop(0, BLOCK, fill, 0)

    return pl.pallas_call(
        kernel,
        out_shape=(
            jax.ShapeDtypeStruct((nodes + 8, slots), jnp.int32),
            jax.ShapeDtypeStruct((most + BLOCK,), jnp.int32),
            jax.ShapeDtypeStruct((1,), jnp.int32),
        ),
        in_specs=[VMEM, SMEM, SMEM],
        out_specs=(VMEM, SMEM, SMEM),
        compiler_params=pltpu.CompilerParams(vmem_limit_bytes=2 << 20),
        name="plan_pairs",
    )(neighbours, neighbour_count, place)


def select_points(blocks, coords, send_rows, send_count, place, after):
    groups = len(blocks)
    chans, points = blocks[0].shape
    width = LANES // groups
    send = send_rows.shape[0] // 2
    unroll = 32

    def kernel(*refs):
        block_refs = refs[:groups]
        coords_ref, rows_ref, count_ref, place_ref = refs[groups : groups + 4]
        own_ref, sent_ref, stack, table, picked = refs[groups + 4 + len(after) :]
        member = place_ref[0]
        side = place_ref[1]
        for step in range(groups):
            base = pl.multiple_of((member ^ step) * width, width)
            empty = jnp.zeros((width - chans, points), jnp.bfloat16)
            stack[pl.ds(base, width), :] = jnp.concatenate([block_refs[step][...], empty], axis=0)
        stack[chans : chans + 3, :] = coords_ref[...]
        stack[chans + 3 : chans + 4, :] = jnp.ones((1, points), jnp.bfloat16)
        own = stack[...].T
        own_ref[...] = own
        table[...] = own.astype(jnp.float32)

        def gather(step, carry):
            base = step * unroll
            first = side * send + base
            rows = [table[pl.ds(rows_ref[first + j], 1), :] for j in range(unroll)]
            for j in range(unroll):
                picked[pl.ds(base + j, 1), :] = rows[j]
            return carry

        lax.fori_loop(0, send // unroll, gather, 0)
        slot = lax.broadcasted_iota(jnp.int32, (send, LANES), 0)
        sent_ref[...] = jnp.where(slot < count_ref[side, 0], picked[...], 0.0).astype(jnp.bfloat16)

    return pl.pallas_call(
        kernel,
        out_shape=(
            jax.ShapeDtypeStruct((points, LANES), jnp.bfloat16),
            jax.ShapeDtypeStruct((send, LANES), jnp.bfloat16),
        ),
        in_specs=[VMEM] * (groups + 1) + [SMEM] * 3 + [ANY] * len(after),
        out_specs=(VMEM, VMEM),
        scratch_shapes=[
            pltpu.VMEM((LANES, points), jnp.bfloat16),
            pltpu.VMEM((points, LANES), jnp.float32),
            pltpu.VMEM((send, LANES), jnp.float32),
        ],
        compiler_params=pltpu.CompilerParams(vmem_limit_bytes=12 << 20),
        name="select_points",
    )(*blocks, coords, send_rows, send_count, place, *after)


def encode(own, other, plan, place, weights, chans, width, depth):
    rows, chunks, total = plan
    table_weight, hidden_weight, out_weight, vectors = weights
    points = own.shape[0]
    send = other.shape[0]
    nodes = rows.shape[0] - 8
    slots = rows.shape[1]
    shift = (slots // CHUNK).bit_length() - 1
    total_rows = points + send
    pairs = BLOCK * CHUNK
    all_nodes = ZD * nodes

    def kernel(
        own_ref, other_ref, rows_ref, list_ref, total_ref, place_ref, table_w, hidden_w, out_w,
        vec_ref, keep_ref, give_ref, table, picked, node_pre, acc, turned,
    ):
        parity = place_ref[1]
        first_id = place_ref[2]

        def fill(source, start, count):
            step = 256
            for at in range(0, count, step):
                both = jnp.dot(source[pl.ds(at, step), :], table_w[...], preferred_element_type=jnp.float32)
                pre = both[:, :LANES].astype(jnp.bfloat16).astype(jnp.float32)
                table[pl.ds(2 * (start + at), step, stride=2), :] = pre
                table[pl.ds(2 * (start + at) + 1, step, stride=2), :] = both[:, LANES:]

        fill(own_ref, 0, points)
        fill(other_ref, points, send)
        table[pl.ds(2 * total_rows, 8), :] = jnp.zeros((8, LANES), jnp.float32)

        vec = vec_ref[...]
        bias_two = vec[4:5]
        bias_three = vec[5:6]
        ids = first_id + lax.broadcasted_iota(jnp.int32, (nodes + 8, 1), 0)
        node_pre[...] = node_term(vec[0:3], vec[3:4], ids, depth)
        acc[...] = jnp.zeros((nodes + 8, LANES), jnp.float32)

        def one_block(index, carry):
            names = [list_ref[index * BLOCK + piece] for piece in range(BLOCK)]
            for piece in range(BLOCK):
                at = names[piece] * CHUNK
                got = [table[pl.ds(rows_ref[at + j], 2), :] for j in range(CHUNK)]
                for j in range(CHUNK):
                    picked[pl.ds(2 * (piece * CHUNK + j), 2), :] = got[j]
            step = 8
            for group in range(BLOCK // step):
                base = group * step * CHUNK
                offset = jnp.concatenate(
                    [
                        jnp.broadcast_to(
                            node_pre[pl.ds(names[group * step + i] >> shift, 1), :], (CHUNK, LANES)
                        )
                        for i in range(step)
                    ],
                    axis=0,
                )
                pre = picked[pl.ds(2 * base, step * CHUNK, stride=2), :]
                val = picked[pl.ds(2 * base + 1, step * CHUNK, stride=2), :]
                first = jax.nn.gelu(pre + offset).astype(jnp.bfloat16)
                second = jnp.dot(first, hidden_w[...], preferred_element_type=jnp.float32)
                second = jax.nn.gelu(second + bias_two).astype(jnp.bfloat16)
                kappa = jnp.dot(second, out_w[...], preferred_element_type=jnp.float32) + bias_three
                product = kappa * val
                for i in range(step):
                    part = jnp.sum(product[i * CHUNK : (i + 1) * CHUNK], axis=0, keepdims=True)
                    spot = pl.ds(names[group * step + i] >> shift, 1)
                    acc[spot, :] = acc[spot, :] + part
            return carry

        lax.fori_loop(0, total_ref[0], one_block, 0)
        sums = acc[0:nodes]
        means = (sums / sums[:, LANES - 1 :]).T
        blank = jnp.zeros((LANES, nodes), jnp.float32)
        low = jnp.where(parity == 1, means, blank)
        turned[...] = jnp.concatenate([low, means - low], axis=1)
        mine = pl.multiple_of((1 - parity) * width, width)
        theirs = pl.multiple_of(parity * width, width)
        keep_ref[...] = turned[pl.ds(mine, chans), :]
        give_ref[...] = turned[pl.ds(theirs, chans), :]

    piece = jax.ShapeDtypeStruct((chans, all_nodes), jnp.float32)
    return pl.pallas_call(
        kernel,
        out_shape=(piece, piece),
        in_specs=[VMEM, VMEM] + [SMEM] * 4 + [VMEM] * 4,
        out_specs=(VMEM, VMEM),
        scratch_shapes=[
            pltpu.VMEM((2 * total_rows + 8, LANES), jnp.float32),
            pltpu.VMEM((2 * pairs, LANES), jnp.float32),
            pltpu.VMEM((nodes + 8, LANES), jnp.float32),
            pltpu.VMEM((nodes + 8, LANES), jnp.float32),
            pltpu.VMEM((LANES, all_nodes), jnp.float32),
        ],
        compiler_params=pltpu.CompilerParams(vmem_limit_bytes=16 << 20),
        name="encode",
    )(
        own, other, rows.reshape(-1), chunks, total, place, table_weight, hidden_weight, out_weight,
        vectors,
    )


def shards(
    features,
    coords,
    send_rows,
    send_count,
    neighbours,
    neighbour_count,
    geom_weight,
    feat_weight,
    bias_one,
    hidden_weight,
    bias_two,
    out_weight,
    bias_three,
):
    groups = lax.axis_size("chan")
    slabs = lax.axis_size("slab")
    member = lax.axis_index("chan")
    slab_id = lax.axis_index("slab")
    depth = ZD * slabs
    chans, points = features.shape
    send = send_rows.shape[1]
    per_slab = neighbours.shape[0]
    hidden = hidden_weight.shape[0]
    nodes = per_slab // ZD
    width = LANES // groups

    blocks = [features]
    for step in range(1, groups):
        blocks.append(lax.ppermute(features, "chan", [(i, i ^ step) for i in range(groups)]))

    plane = member % 2
    start = plane * nodes
    upper = 1 - plane
    place = jnp.stack([member, upper, slab_id * per_slab + start, start]).astype(jnp.int32)
    plan = plan_pairs(neighbours, neighbour_count, place, nodes, points, send)

    def lanes_of(weight):
        lead = weight.shape[:-1]
        split = weight.reshape(lead + (groups, chans))
        return jnp.pad(split, [(0, 0)] * len(lead) + [(0, 0), (0, width - chans)]).reshape(lead + (LANES,))

    first_lane = (member // 2) * 2 * width

    def pair_of(weight):
        part = lax.dynamic_slice_in_dim(lanes_of(weight), first_lane, 2 * width, weight.ndim - 1)
        return jnp.pad(part, [(0, 0)] * (weight.ndim - 1) + [(0, LANES - 2 * width)])

    row = jnp.arange(LANES)[:, None]
    lane = jnp.arange(LANES)[None, :]
    take = ((row == first_lane + lane) & (lane < 2 * width)) | ((row == chans + 3) & (lane == LANES - 1))
    geom = jnp.pad(geom_weight[:, 3:6], ((0, 0), (chans, LANES - chans - 3)))
    pre_weight = jnp.pad((lanes_of(feat_weight) + geom).T, ((0, 0), (0, LANES - hidden)))
    table_weight = jnp.concatenate([pre_weight, take.astype(jnp.bfloat16)], axis=1)
    hidden_t = jnp.pad(hidden_weight.T, ((0, LANES - hidden), (0, LANES - hidden)))
    out_t = jnp.pad(pair_of(out_weight.T), ((0, LANES - hidden), (0, 0)))
    tail = (0, LANES - hidden)
    vectors = jnp.concatenate(
        [
            jnp.pad(geom_weight[:, 0:3].astype(jnp.float32).T, ((0, 0), tail)),
            jnp.pad(bias_one, tail)[None],
            jnp.pad(bias_two, tail)[None],
            pair_of(bias_three)[None] + (lane == LANES - 1),
            jnp.zeros((2, LANES), jnp.float32),
        ],
        axis=0,
    )
    weights = (table_weight, hidden_t, out_t, vectors)

    own, sent = select_points(
        blocks, coords, send_rows.reshape(-1), send_count, place, plan + weights
    )
    moves = []
    for slab in range(slabs):
        for who in range(groups):
            target = slab + 1 if who % 2 == 0 else slab - 1
            if 0 <= target < slabs:
                moves.append((slab * groups + who, target * groups + who))
    other = lax.ppermute(sent, ("slab", "chan"), moves)
    keep, give = encode(own, other, plan, place, weights, chans, width, depth)
    return keep + lax.ppermute(give, "chan", [(i, i ^ 1) for i in range(groups)])


def solution(mesh):
    placed = (
        P("chan", "slab"),
        P(None, "slab"),
        P(None, "slab"),
        P(None, "slab"),
        P("slab", None),
        P("slab"),
        P(),
        P(),
        P(),
        P(),
        P(),
        P(),
        P(),
    )
    return jax.shard_map(
        shards, mesh=mesh, in_specs=placed, out_specs=P("chan", "slab"), check_vma=False
    )
```

```python
import jax
import jax.numpy as jnp
from jax import lax
from jax.experimental import pallas as pl
from jax.experimental.pallas import tpu as pltpu
from jax.sharding import PartitionSpec as P

ZD = 2
GX = 16
GY = 4
LANES = 128
CHUNK = 16
BLOCK = 64
CONSTANT = 16.0
GELU_ONE = 0.7978845608028654
GELU_CUBE = 0.044715 * GELU_ONE

SMEM = pl.BlockSpec(memory_space=pltpu.SMEM)
VMEM = pl.BlockSpec(memory_space=pltpu.VMEM)
ANY = pl.BlockSpec(memory_space=pl.ANY)
HBM = pl.BlockSpec(memory_space=pltpu.MemorySpace.HBM)


def gelu_doubled(x):
    inner = x * (GELU_ONE + GELU_CUBE * (x * x))
    return x * (1.0 + jnp.tanh(inner))


def prepare(
    neighbours, neighbour_count, geom_weight, feat_weight, bias_one, hidden_weight, bias_two,
    out_weight, bias_three, place, groups, points, send, depth,
):
    per_slab, slots = neighbours.shape
    hidden, channels = feat_weight.shape
    chans = channels // groups
    width = LANES // groups
    nodes = per_slab // ZD
    per_node = slots // CHUNK
    most = nodes * per_node
    nothing = 2 * (points + send)
    extra = slice(hidden, hidden + 3)

    def parts(value):
        high = value.astype(jnp.bfloat16).astype(jnp.float32)
        mid = (value - high).astype(jnp.bfloat16).astype(jnp.float32)
        low = (value - high - mid).astype(jnp.bfloat16).astype(jnp.float32)
        return jnp.concatenate([high, mid, low], axis=0) * (1.0 / CONSTANT)

    given = (
        neighbour_count, neighbours, geom_weight.T, feat_weight, bias_one[None], hidden_weight,
        bias_two[None], out_weight.T, bias_three[None],
    )

    def kernel(*refs):
        place_ref = refs[len(given)]
        rows_ref, list_ref, total_ref, table_w, hidden_w, out_w, node_pre = refs[len(given) + 1 :][:7]
        held = refs[len(given) + 8 :][: len(given)]
        wide, square, spread, arrived = refs[2 * len(given) + 8 :]
        copies = [
            pltpu.make_async_copy(source, target, arrived.at[at])
            for at, (source, target) in enumerate(zip(refs, held))
        ]
        for copy in copies:
            copy.start()
        for copy in copies:
            copy.wait()
        count_ref, nbr_ref, geom_ref, feat_ref, one_ref, hidden_ref, two_ref, out_ref, three_ref = held
        member = place_ref[0]
        first_id = place_ref[2]
        start = place_ref[3]
        lane = lax.broadcasted_iota(jnp.int32, (1, LANES), 1)

        def one_node(node, at):
            count = count_ref[start + node]
            row = nbr_ref[pl.ds(start + node, 1), :]
            row = jnp.where(row >= points + send, row - send, row)
            slot = lax.broadcasted_iota(jnp.int32, (1, slots), 1)
            rows_ref[pl.ds(node, 1), :] = jnp.where(slot < count, 2 * row, nothing)
            for piece in range(per_node):
                list_ref[at + piece] = node * per_node + piece
            return at + (count + CHUNK - 1) // CHUNK

        used = lax.fori_loop(0, nodes, one_node, 0)
        rows_ref[pl.ds(nodes, 8), :] = jnp.full((8, slots), nothing, jnp.int32)
        total_ref[0] = (used + BLOCK - 1) // BLOCK

        def fill(step, carry):
            list_ref[used + step] = most
            return carry

        lax.fori_loop(0, BLOCK, fill, 0)

        square[...] = jnp.zeros((LANES, LANES), jnp.float32)
        square[0:hidden, 0:channels] = feat_ref[...].astype(jnp.float32)
        square[...] = square[...].T
        wide[...] = jnp.zeros((LANES, 2 * LANES), jnp.float32)
        for block in range(groups):
            wide[block * width : block * width + chans, 0:LANES] = square[
                block * chans : (block + 1) * chans, :
            ]
        geom = geom_ref[...].astype(jnp.float32)
        wide[chans : chans + 3, 0:hidden] = geom[3:6]
        row = lax.broadcasted_iota(jnp.int32, (LANES, LANES), 0)
        col = lax.broadcasted_iota(jnp.int32, (LANES, LANES), 1)
        pair = member // 2
        take = ((row == pair * 2 * width + col) & (col < 2 * width)) | (
            (row == chans + 3) & (col == LANES - 1)
        )
        wide[:, LANES:] = take.astype(jnp.float32)
        table_w[...] = wide[...].astype(jnp.bfloat16)

        square[...] = jnp.zeros((LANES, LANES), jnp.float32)
        square[0:hidden, 0:hidden] = 0.5 * hidden_ref[...].astype(jnp.float32)
        square[...] = square[...].T
        square[extra, 0:hidden] = parts(two_ref[...])
        ones = (lane >= hidden) & (lane < hidden + 3)
        square[hidden : hidden + 1, hidden:] = jnp.where(ones, 0.5, 0.0)[:, hidden:]
        hidden_w[...] = square[...].astype(jnp.bfloat16)

        square[...] = jnp.zeros((LANES, LANES), jnp.float32)
        square[0:hidden, 0:channels] = 0.5 * out_ref[...].astype(jnp.float32)
        square[extra, 0:channels] = parts(three_ref[...])
        square[...] = square[...].T
        spread[...] = jnp.zeros((LANES, LANES), jnp.float32)
        for half in range(2):
            spread[half * width : half * width + chans, :] = square[
                pl.ds((2 * pair + half) * chans, chans), :
            ]
        spread[LANES - 1 :, :] = jnp.where(lane == hidden, 1.0 / CONSTANT, 0.0)
        out_w[...] = spread[...].T.astype(jnp.bfloat16)

        ids = first_id + lax.broadcasted_iota(jnp.int32, (nodes + 8, 1), 0)
        along_x = ((ids % GX).astype(jnp.float32) + 0.5) / GX
        along_y = ((ids // GX % GY).astype(jnp.float32) + 0.5) / GY
        along_z = ((ids // (GX * GY)).astype(jnp.float32) + 0.5) / depth
        term = geom[0:1] * along_x + geom[1:2] * along_y + geom[2:3] * along_z + one_ref[...]
        node_pre[...] = jnp.broadcast_to(jnp.where(ones, 0.5 * CONSTANT, 0.0), (nodes + 8, LANES))
        node_pre[:, 0:hidden] = term

    out = pl.pallas_call(
        kernel,
        out_shape=(
            jax.ShapeDtypeStruct((nodes + 8, slots), jnp.int32),
            jax.ShapeDtypeStruct((most + BLOCK,), jnp.int32),
            jax.ShapeDtypeStruct((1,), jnp.int32),
            jax.ShapeDtypeStruct((LANES, 2 * LANES), jnp.bfloat16),
            jax.ShapeDtypeStruct((LANES, LANES), jnp.bfloat16),
            jax.ShapeDtypeStruct((LANES, LANES), jnp.bfloat16),
            jax.ShapeDtypeStruct((nodes + 8, LANES), jnp.float32),
        ),
        in_specs=[HBM] * len(given) + [SMEM],
        out_specs=(VMEM, SMEM, SMEM) + (VMEM,) * 4,
        scratch_shapes=[pltpu.SMEM(neighbour_count.shape, jnp.int32)]
        + [pltpu.VMEM(array.shape, array.dtype) for array in given[1:]]
        + [
            pltpu.VMEM((LANES, 2 * LANES), jnp.float32),
            pltpu.VMEM((LANES, LANES), jnp.float32),
            pltpu.VMEM((LANES, LANES), jnp.float32),
            pltpu.SemaphoreType.DMA((len(given),)),
        ],
        name="prepare",
    )(*given, place)
    return out[:3], out[3:]


def select_points(blocks, coords, send_rows, send_count, place, after):
    groups = len(blocks)
    chans, points = blocks[0].shape
    width = LANES // groups
    send = send_rows.shape[0] // 2
    unroll = 32

    def kernel(*refs):
        block_refs = refs[:groups]
        coords_ref, rows_ref, count_ref, place_ref = refs[groups : groups + 4]
        own_ref, sent_ref, stack, table, picked = refs[groups + 4 + len(after) :]
        member = place_ref[0]
        side = place_ref[1]
        for step in range(groups):
            base = pl.multiple_of((member ^ step) * width, width)
            empty = jnp.zeros((width - chans, points), jnp.bfloat16)
            stack[pl.ds(base, width), :] = jnp.concatenate([block_refs[step][...], empty], axis=0)
        stack[chans : chans + 3, :] = coords_ref[...]
        stack[chans + 3 : chans + 4, :] = jnp.ones((1, points), jnp.bfloat16)
        own = stack[...].T
        own_ref[...] = own
        table[...] = own.astype(jnp.float32)

        def gather(step, carry):
            base = step * unroll
            names = rows_ref.at[pl.ds(side * send + base, unroll)]
            rows = [table[pl.ds(names[j], 1), :] for j in range(unroll)]
            for j in range(unroll):
                picked[pl.ds(base + j, 1), :] = rows[j]
            return carry

        lax.fori_loop(0, send // unroll, gather, 0)
        slot = lax.broadcasted_iota(jnp.int32, (send, LANES), 0)
        sent_ref[...] = jnp.where(slot < count_ref[side, 0], picked[...], 0.0).astype(jnp.bfloat16)

    return pl.pallas_call(
        kernel,
        out_shape=(
            jax.ShapeDtypeStruct((points, LANES), jnp.bfloat16),
            jax.ShapeDtypeStruct((send, LANES), jnp.bfloat16),
        ),
        in_specs=[VMEM] * (groups + 1) + [SMEM] * 3 + [ANY] * len(after),
        out_specs=(VMEM, VMEM),
        scratch_shapes=[
            pltpu.VMEM((LANES, points), jnp.bfloat16),
            pltpu.VMEM((points, LANES), jnp.float32),
            pltpu.VMEM((send, LANES), jnp.float32),
        ],
        compiler_params=pltpu.CompilerParams(vmem_limit_bytes=12 << 20),
        name="select_points",
    )(*blocks, coords, send_rows, send_count, place, *after)


def encode(own, other, plan, place, weights, chans, width):
    rows, chunks, total = plan
    table_weight, hidden_weight, out_weight, node_part = weights
    points = own.shape[0]
    send = other.shape[0]
    nodes = rows.shape[0] - 8
    slots = rows.shape[1]
    shift = (slots // CHUNK).bit_length() - 1
    total_rows = points + send
    pairs = BLOCK * CHUNK

    def kernel(
        own_ref, other_ref, rows_ref, list_ref, total_ref, place_ref, table_w, hidden_w, out_w,
        node_pre, keep_ref, give_ref, table, picked, acc, turned,
    ):
        parity = place_ref[1]

        def fill(source, start, count):
            step = 256
            for at in range(0, count, step):
                both = jnp.dot(source[pl.ds(at, step), :], table_w[...], preferred_element_type=jnp.float32)
                pre = both[:, :LANES].astype(jnp.bfloat16).astype(jnp.float32)
                table[pl.ds(2 * (start + at), step, stride=2), :] = pre
                table[pl.ds(2 * (start + at) + 1, step, stride=2), :] = both[:, LANES:]

        fill(own_ref, 0, points)
        fill(other_ref, points, send)
        table[pl.ds(2 * total_rows, 8), :] = jnp.zeros((8, LANES), jnp.float32)
        acc[...] = jnp.zeros((nodes + 8, 8, LANES), jnp.float32)

        def one_block(index, carry):
            ids = list_ref.at[pl.ds(index * BLOCK, BLOCK)]
            names = [ids[piece] for piece in range(BLOCK)]
            for piece in range(BLOCK):
                where = rows_ref.at[pl.ds(names[piece] * CHUNK, CHUNK)]
                got = [table[pl.ds(where[j], 2), :] for j in range(CHUNK)]
                for j in range(CHUNK):
                    picked[pl.ds(2 * (piece * CHUNK + j), 2), :] = got[j]
            step = 8
            for group in range(BLOCK // step):
                base = group * step * CHUNK
                spots = [names[group * step + i] >> shift for i in range(step)]
                offset = jnp.concatenate(
                    [jnp.broadcast_to(node_pre[pl.ds(spot, 1), :], (CHUNK, LANES)) for spot in spots],
                    axis=0,
                )
                pre = picked[pl.ds(2 * base, step * CHUNK, stride=2), :]
                val = picked[pl.ds(2 * base + 1, step * CHUNK, stride=2), :]
                first = gelu_doubled(pre + offset).astype(jnp.bfloat16)
                second = jnp.dot(first, hidden_w[...], preferred_element_type=jnp.float32)
                second = gelu_doubled(second).astype(jnp.bfloat16)
                kappa = jnp.dot(second, out_w[...], preferred_element_type=jnp.float32)
                product = kappa * val
                for i, spot in enumerate(spots):
                    low = product[i * CHUNK : i * CHUNK + 8]
                    for j in range(8, CHUNK, 8):
                        low = low + product[i * CHUNK + j : i * CHUNK + j + 8]
                    acc[spot] = acc[spot] + low
            return carry

        lax.fori_loop(0, total_ref[0], one_block, 0)
        sums = jnp.sum(acc[0:nodes], axis=1)
        means = (sums / sums[:, LANES - 1 :]).T
        low = jnp.where(parity == 1, means, 0.0)
        turned[...] = jnp.concatenate([low, means - low], axis=1)
        mine = pl.multiple_of((1 - parity) * width, width)
        theirs = pl.multiple_of(parity * width, width)
        keep_ref[...] = turned[pl.ds(mine, chans), :]
        give_ref[...] = turned[pl.ds(theirs, chans), :]

    piece = jax.ShapeDtypeStruct((chans, ZD * nodes), jnp.float32)
    return pl.pallas_call(
        kernel,
        out_shape=(piece, piece),
        in_specs=[VMEM, VMEM] + [SMEM] * 4 + [VMEM] * 4,
        out_specs=(VMEM, VMEM),
        scratch_shapes=[
            pltpu.VMEM((2 * total_rows + 8, LANES), jnp.float32),
            pltpu.VMEM((2 * pairs, LANES), jnp.float32),
            pltpu.VMEM((nodes + 8, 8, LANES), jnp.float32),
            pltpu.VMEM((LANES, ZD * nodes), jnp.float32),
        ],
        compiler_params=pltpu.CompilerParams(vmem_limit_bytes=16 << 20),
        name="encode",
    )(
        own, other, rows.reshape(-1), chunks, total, place, table_weight, hidden_weight, out_weight,
        node_part,
    )


def shards(
    features,
    coords,
    send_rows,
    send_count,
    neighbours,
    neighbour_count,
    geom_weight,
    feat_weight,
    bias_one,
    hidden_weight,
    bias_two,
    out_weight,
    bias_three,
):
    groups = lax.axis_size("chan")
    slabs = lax.axis_size("slab")
    member = lax.axis_index("chan")
    slab_id = lax.axis_index("slab")
    chans, points = features.shape
    send = send_rows.shape[1]
    per_slab = neighbours.shape[0]
    nodes = per_slab // ZD
    width = LANES // groups

    blocks = [features]
    for step in range(1, groups):
        blocks.append(lax.ppermute(features, "chan", [(i, i ^ step) for i in range(groups)]))

    plane = member % 2
    start = plane * nodes
    upper = 1 - plane
    place = jnp.stack([member, upper, slab_id * per_slab + start, start]).astype(jnp.int32)
    plan, weights = prepare(
        neighbours, neighbour_count, geom_weight, feat_weight, bias_one, hidden_weight, bias_two,
        out_weight, bias_three, place, groups, points, send, ZD * slabs,
    )
    own, sent = select_points(
        blocks, coords, send_rows.reshape(-1), send_count, place, plan + weights
    )
    moves = []
    for slab in range(slabs):
        for who in range(groups):
            target = slab + 1 if who % 2 == 0 else slab - 1
            if 0 <= target < slabs:
                moves.append((slab * groups + who, target * groups + who))
    other = lax.ppermute(sent, ("slab", "chan"), moves)
    keep, give = encode(own, other, plan, place, weights, chans, width)
    return keep + lax.ppermute(give, "chan", [(i, i ^ 1) for i in range(groups)])


def solution(mesh):
    placed = (
        P("chan", "slab"),
        P(None, "slab"),
        P(None, "slab"),
        P(None, "slab"),
        P("slab", None),
        P("slab"),
        P(),
        P(),
        P(),
        P(),
        P(),
        P(),
        P(),
    )
    return jax.shard_map(
        shards, mesh=mesh, in_specs=placed, out_specs=P("chan", "slab"), check_vma=False
    )
```

```python
import jax
import jax.numpy as jnp
from jax import lax
from jax.experimental import pallas as pl
from jax.experimental.pallas import tpu as pltpu
from jax.sharding import PartitionSpec as P

ZD = 2
GX = 16
GY = 4
LANES = 128
CHUNK = 16
BLOCK = 64
CONSTANT = 16.0
GELU_ONE = 0.7978845608028654
GELU_CUBE = 0.044715 * GELU_ONE

SMEM = pl.BlockSpec(memory_space=pltpu.SMEM)
VMEM = pl.BlockSpec(memory_space=pltpu.VMEM)
ANY = pl.BlockSpec(memory_space=pl.ANY)
HBM = pl.BlockSpec(memory_space=pltpu.MemorySpace.HBM)


def gelu_doubled(x):
    inner = x * (GELU_ONE + GELU_CUBE * (x * x))
    return x * (1.0 + jnp.tanh(inner))


def prepare(
    neighbours, neighbour_count, geom_weight, feat_weight, bias_one, hidden_weight, bias_two,
    out_weight, bias_three, place, groups, points, send, depth,
):
    per_slab, slots = neighbours.shape
    hidden, channels = feat_weight.shape
    chans = channels // groups
    width = LANES // groups
    nodes = per_slab // ZD
    per_node = slots // CHUNK
    most = nodes * per_node
    nothing = 2 * (points + send)
    extra = slice(hidden, hidden + 3)

    def parts(value):
        high = value.astype(jnp.bfloat16).astype(jnp.float32)
        mid = (value - high).astype(jnp.bfloat16).astype(jnp.float32)
        low = (value - high - mid).astype(jnp.bfloat16).astype(jnp.float32)
        return jnp.concatenate([high, mid, low], axis=0) * (1.0 / CONSTANT)

    given = (
        neighbour_count, neighbours, geom_weight.T, feat_weight, bias_one[None], hidden_weight,
        bias_two[None], out_weight.T, bias_three[None],
    )

    def kernel(*refs):
        place_ref = refs[len(given)]
        rows_ref, list_ref, total_ref, table_w, hidden_w, out_w, node_pre = refs[len(given) + 1 :][:7]
        held = refs[len(given) + 8 :][: len(given)]
        wide, square, spread, arrived = refs[2 * len(given) + 8 :]
        copies = [
            pltpu.make_async_copy(source, target, arrived.at[at])
            for at, (source, target) in enumerate(zip(refs, held))
        ]
        for copy in copies:
            copy.start()
        for copy in copies:
            copy.wait()
        count_ref, nbr_ref, geom_ref, feat_ref, one_ref, hidden_ref, two_ref, out_ref, three_ref = held
        member = place_ref[0]
        first_id = place_ref[2]
        start = place_ref[3]
        lane = lax.broadcasted_iota(jnp.int32, (1, LANES), 1)

        def one_node(node, at):
            count = count_ref[start + node]
            row = nbr_ref[pl.ds(start + node, 1), :]
            row = jnp.where(row >= points + send, row - send, row)
            slot = lax.broadcasted_iota(jnp.int32, (1, slots), 1)
            rows_ref[pl.ds(node, 1), :] = jnp.where(slot < count, 2 * row, nothing)
            for piece in range(per_node):
                list_ref[at + piece] = node * per_node + piece
            return at + (count + CHUNK - 1) // CHUNK

        used = lax.fori_loop(0, nodes, one_node, 0)
        rows_ref[pl.ds(nodes, 8), :] = jnp.full((8, slots), nothing, jnp.int32)
        total_ref[0] = (used + BLOCK - 1) // BLOCK

        def fill(step, carry):
            list_ref[used + step] = most
            return carry

        lax.fori_loop(0, BLOCK, fill, 0)

        square[...] = jnp.zeros((LANES, LANES), jnp.float32)
        square[0:hidden, 0:channels] = feat_ref[...].astype(jnp.float32)
        square[...] = square[...].T
        wide[...] = jnp.zeros((LANES, 2 * LANES), jnp.float32)
        for block in range(groups):
            wide[block * width : block * width + chans, 0:LANES] = square[
                block * chans : (block + 1) * chans, :
            ]
        geom = geom_ref[...].astype(jnp.float32)
        wide[chans : chans + 3, 0:hidden] = geom[3:6]
        row = lax.broadcasted_iota(jnp.int32, (LANES, LANES), 0)
        col = lax.broadcasted_iota(jnp.int32, (LANES, LANES), 1)
        pair = member // 2
        take = ((row == pair * 2 * width + col) & (col < 2 * width)) | (
            (row == chans + 3) & (col == LANES - 1)
        )
        wide[:, LANES:] = take.astype(jnp.float32)
        table_w[...] = wide[...].astype(jnp.bfloat16)

        square[...] = jnp.zeros((LANES, LANES), jnp.float32)
        square[0:hidden, 0:hidden] = 0.5 * hidden_ref[...].astype(jnp.float32)
        square[...] = square[...].T
        square[extra, 0:hidden] = parts(two_ref[...])
        ones = (lane >= hidden) & (lane < hidden + 3)
        square[hidden : hidden + 1, hidden:] = jnp.where(ones, 0.5, 0.0)[:, hidden:]
        hidden_w[...] = square[...].astype(jnp.bfloat16)

        square[...] = jnp.zeros((LANES, LANES), jnp.float32)
        square[0:hidden, 0:channels] = 0.5 * out_ref[...].astype(jnp.float32)
        square[extra, 0:channels] = parts(three_ref[...])
        square[...] = square[...].T
        spread[...] = jnp.zeros((LANES, LANES), jnp.float32)
        for half in range(2):
            spread[half * width : half * width + chans, :] = square[
                pl.ds((2 * pair + half) * chans, chans), :
            ]
        spread[LANES - 1 :, :] = jnp.where(lane == hidden, 1.0 / CONSTANT, 0.0)
        out_w[...] = spread[...].T.astype(jnp.bfloat16)

        ids = first_id + lax.broadcasted_iota(jnp.int32, (nodes + 8, 1), 0)
        along_x = ((ids % GX).astype(jnp.float32) + 0.5) / GX
        along_y = ((ids // GX % GY).astype(jnp.float32) + 0.5) / GY
        along_z = ((ids // (GX * GY)).astype(jnp.float32) + 0.5) / depth
        term = geom[0:1] * along_x + geom[1:2] * along_y + geom[2:3] * along_z + one_ref[...]
        node_pre[...] = jnp.broadcast_to(jnp.where(ones, 0.5 * CONSTANT, 0.0), (nodes + 8, LANES))
        node_pre[:, 0:hidden] = term

    out = pl.pallas_call(
        kernel,
        out_shape=(
            jax.ShapeDtypeStruct((nodes + 8, slots), jnp.int32),
            jax.ShapeDtypeStruct((most + BLOCK,), jnp.int32),
            jax.ShapeDtypeStruct((1,), jnp.int32),
            jax.ShapeDtypeStruct((LANES, 2 * LANES), jnp.bfloat16),
            jax.ShapeDtypeStruct((LANES, LANES), jnp.bfloat16),
            jax.ShapeDtypeStruct((LANES, LANES), jnp.bfloat16),
            jax.ShapeDtypeStruct((nodes + 8, LANES), jnp.float32),
        ),
        in_specs=[HBM] * len(given) + [SMEM],
        out_specs=(VMEM, SMEM, SMEM) + (VMEM,) * 4,
        scratch_shapes=[pltpu.SMEM(neighbour_count.shape, jnp.int32)]
        + [pltpu.VMEM(array.shape, array.dtype) for array in given[1:]]
        + [
            pltpu.VMEM((LANES, 2 * LANES), jnp.float32),
            pltpu.VMEM((LANES, LANES), jnp.float32),
            pltpu.VMEM((LANES, LANES), jnp.float32),
            pltpu.SemaphoreType.DMA((len(given),)),
        ],
        name="prepare",
    )(*given, place)
    return out[:3], out[3:]


def select_points(blocks, coords, send_rows, send_count, place, after):
    groups = len(blocks)
    chans, points = blocks[0].shape
    width = LANES // groups
    send = send_rows.shape[0] // 2
    unroll = 32

    def kernel(*refs):
        block_refs = refs[:groups]
        coords_ref, rows_ref, count_ref, place_ref = refs[groups : groups + 4]
        own_ref, sent_ref, stack, table, picked = refs[groups + 4 + len(after) :]
        member = place_ref[0]
        side = place_ref[1]
        for step in range(groups):
            base = pl.multiple_of((member ^ step) * width, width)
            empty = jnp.zeros((width - chans, points), jnp.bfloat16)
            stack[pl.ds(base, width), :] = jnp.concatenate([block_refs[step][...], empty], axis=0)
        stack[chans : chans + 3, :] = coords_ref[...]
        stack[chans + 3 : chans + 4, :] = jnp.ones((1, points), jnp.bfloat16)
        own = stack[...].T
        own_ref[...] = own
        table[...] = own.astype(jnp.float32)

        def gather(step, carry):
            base = step * unroll
            names = rows_ref.at[pl.ds(side * send + base, unroll)]
            rows = [table[pl.ds(names[j], 1), :] for j in range(unroll)]
            for j in range(unroll):
                picked[pl.ds(base + j, 1), :] = rows[j]
            return carry

        lax.fori_loop(0, send // unroll, gather, 0)
        slot = lax.broadcasted_iota(jnp.int32, (send, LANES), 0)
        sent_ref[...] = jnp.where(slot < count_ref[side, 0], picked[...], 0.0).astype(jnp.bfloat16)

    return pl.pallas_call(
        kernel,
        out_shape=(
            jax.ShapeDtypeStruct((points, LANES), jnp.bfloat16),
            jax.ShapeDtypeStruct((send, LANES), jnp.bfloat16),
        ),
        in_specs=[VMEM] * (groups + 1) + [SMEM] * 3 + [ANY] * len(after),
        out_specs=(VMEM, VMEM),
        scratch_shapes=[
            pltpu.VMEM((LANES, points), jnp.bfloat16),
            pltpu.VMEM((points, LANES), jnp.float32),
            pltpu.VMEM((send, LANES), jnp.float32),
        ],
        compiler_params=pltpu.CompilerParams(vmem_limit_bytes=12 << 20),
        name="select_points",
    )(*blocks, coords, send_rows, send_count, place, *after)


def encode(own, other, plan, place, weights, chans, width):
    rows, chunks, total = plan
    table_weight, hidden_weight, out_weight, node_part = weights
    points = own.shape[0]
    send = other.shape[0]
    nodes = rows.shape[0] - 8
    slots = rows.shape[1]
    shift = (slots // CHUNK).bit_length() - 1
    total_rows = points + send
    pairs = BLOCK * CHUNK

    def kernel(
        own_ref, other_ref, rows_ref, list_ref, total_ref, place_ref, table_w, hidden_w, out_w,
        node_pre, keep_ref, give_ref, table, picked, acc, turned,
    ):
        parity = place_ref[1]

        def fill(source, start, count):
            step = 256
            for at in range(0, count, step):
                both = jnp.dot(source[pl.ds(at, step), :], table_w[...], preferred_element_type=jnp.float32)
                pre = both[:, :LANES].astype(jnp.bfloat16).astype(jnp.float32)
                table[pl.ds(2 * (start + at), step, stride=2), :] = pre
                table[pl.ds(2 * (start + at) + 1, step, stride=2), :] = both[:, LANES:]

        fill(own_ref, 0, points)
        fill(other_ref, points, send)
        table[pl.ds(2 * total_rows, 8), :] = jnp.zeros((8, LANES), jnp.float32)
        acc[...] = jnp.zeros((nodes + 8, 8, LANES), jnp.float32)

        def one_block(index, carry):
            ids = list_ref.at[pl.ds(index * BLOCK, BLOCK)]
            names = [ids[piece] for piece in range(BLOCK)]
            for piece in range(BLOCK):
                where = rows_ref.at[pl.ds(names[piece] * CHUNK, CHUNK)]
                got = [table[pl.ds(where[j], 2), :] for j in range(CHUNK)]
                for j in range(CHUNK):
                    picked[pl.ds(2 * (piece * CHUNK + j), 2), :] = got[j]
            step = 8
            for group in range(BLOCK // step):
                base = group * step * CHUNK
                spots = [names[group * step + i] >> shift for i in range(step)]
                offset = jnp.concatenate(
                    [jnp.broadcast_to(node_pre[pl.ds(spot, 1), :], (CHUNK, LANES)) for spot in spots],
                    axis=0,
                )
                pre = picked[pl.ds(2 * base, step * CHUNK, stride=2), :]
                val = picked[pl.ds(2 * base + 1, step * CHUNK, stride=2), :]
                first = gelu_doubled(pre + offset).astype(jnp.bfloat16)
                second = jnp.dot(first, hidden_w[...], preferred_element_type=jnp.float32)
                second = gelu_doubled(second).astype(jnp.bfloat16)
                kappa = jnp.dot(second, out_w[...], preferred_element_type=jnp.float32)
                product = kappa * val
                for i, spot in enumerate(spots):
                    low = product[i * CHUNK : i * CHUNK + 8]
                    for j in range(8, CHUNK, 8):
                        low = low + product[i * CHUNK + j : i * CHUNK + j + 8]
                    acc[spot] = acc[spot] + low
            return carry

        lax.fori_loop(0, total_ref[0], one_block, 0)
        sums = jnp.sum(acc[0:nodes], axis=1)
        means = (sums / sums[:, LANES - 1 :]).T
        low = jnp.where(parity == 1, means, 0.0)
        turned[...] = jnp.concatenate([low, means - low], axis=1)
        mine = pl.multiple_of((1 - parity) * width, width)
        theirs = pl.multiple_of(parity * width, width)
        keep_ref[...] = turned[pl.ds(mine, chans), :]
        give_ref[...] = turned[pl.ds(theirs, chans), :]

    piece = jax.ShapeDtypeStruct((chans, ZD * nodes), jnp.float32)
    return pl.pallas_call(
        kernel,
        out_shape=(piece, piece),
        in_specs=[VMEM, VMEM] + [SMEM] * 4 + [VMEM] * 4,
        out_specs=(VMEM, VMEM),
        scratch_shapes=[
            pltpu.VMEM((2 * total_rows + 8, LANES), jnp.float32),
            pltpu.VMEM((2 * pairs, LANES), jnp.float32),
            pltpu.VMEM((nodes + 8, 8, LANES), jnp.float32),
            pltpu.VMEM((LANES, ZD * nodes), jnp.float32),
        ],
        compiler_params=pltpu.CompilerParams(vmem_limit_bytes=16 << 20),
        name="encode",
    )(
        own, other, rows.reshape(-1), chunks, total, place, table_weight, hidden_weight, out_weight,
        node_part,
    )


def shards(
    features,
    coords,
    send_rows,
    send_count,
    neighbours,
    neighbour_count,
    geom_weight,
    feat_weight,
    bias_one,
    hidden_weight,
    bias_two,
    out_weight,
    bias_three,
):
    groups = lax.axis_size("chan")
    slabs = lax.axis_size("slab")
    member = lax.axis_index("chan")
    slab_id = lax.axis_index("slab")
    chans, points = features.shape
    send = send_rows.shape[1]
    per_slab = neighbours.shape[0]
    nodes = per_slab // ZD
    width = LANES // groups

    blocks = [features]
    for step in range(1, groups):
        blocks.append(lax.ppermute(features, "chan", [(i, i ^ step) for i in range(groups)]))

    plane = member % 2
    start = plane * nodes
    upper = 1 - plane
    place = jnp.stack([member, upper, slab_id * per_slab + start, start]).astype(jnp.int32)
    plan, weights = prepare(
        neighbours, neighbour_count, geom_weight, feat_weight, bias_one, hidden_weight, bias_two,
        out_weight, bias_three, place, groups, points, send, ZD * slabs,
    )
    own, sent = select_points(
        blocks, coords, send_rows.reshape(-1), send_count, place, plan[2:]
    )
    moves = []
    for slab in range(slabs):
        for who in range(groups):
            target = slab + 1 if who % 2 == 0 else slab - 1
            if 0 <= target < slabs:
                moves.append((slab * groups + who, target * groups + who))
    other = lax.ppermute(sent, ("slab", "chan"), moves)
    keep, give = encode(own, other, plan, place, weights, chans, width)
    return keep + lax.ppermute(give, "chan", [(i, i ^ 1) for i in range(groups)])


def solution(mesh):
    placed = (
        P("chan", "slab"),
        P(None, "slab"),
        P(None, "slab"),
        P(None, "slab"),
        P("slab", None),
        P("slab"),
        P(),
        P(),
        P(),
        P(),
        P(),
        P(),
        P(),
    )
    return jax.shard_map(
        shards, mesh=mesh, in_specs=placed, out_specs=P("chan", "slab"), check_vma=False
    )
```

```python
import jax
import jax.numpy as jnp
from jax import lax
from jax.experimental import pallas as pl
from jax.experimental.pallas import tpu as pltpu
from jax.sharding import PartitionSpec as P

ZD = 2
GX = 16
GY = 4
LANES = 128
CHUNK = 16
BLOCK = 64
CONSTANT = 16.0
GELU_ONE = 0.7978845608028654
GELU_CUBE = 0.044715 * GELU_ONE

SMEM = pl.BlockSpec(memory_space=pltpu.SMEM)
VMEM = pl.BlockSpec(memory_space=pltpu.VMEM)
HBM = pl.BlockSpec(memory_space=pltpu.MemorySpace.HBM)


def gelu_doubled(x):
    inner = x * (GELU_ONE + GELU_CUBE * (x * x))
    return x * (1.0 + jnp.tanh(inner))


def prepare(
    neighbours, neighbour_count, geom_weight, feat_weight, bias_one, hidden_weight, bias_two,
    out_weight, bias_three, place, groups, points, send_rows, depth,
):
    per_slab, slots = neighbours.shape
    send = send_rows.shape[1]
    hidden, channels = feat_weight.shape
    chans = channels // groups
    width = LANES // groups
    nodes = per_slab // ZD
    per_node = slots // CHUNK
    most = nodes * per_node
    nothing = 2 * (points + send)
    extra = slice(hidden, hidden + 3)

    def parts(value):
        high = value.astype(jnp.bfloat16).astype(jnp.float32)
        mid = (value - high).astype(jnp.bfloat16).astype(jnp.float32)
        low = (value - high - mid).astype(jnp.bfloat16).astype(jnp.float32)
        return jnp.concatenate([high, mid, low], axis=0) * (1.0 / CONSTANT)

    given = (
        neighbour_count, neighbours, geom_weight.T, feat_weight, bias_one[None], hidden_weight,
        bias_two[None], out_weight.T, bias_three[None], send_rows,
    )
    tall = most * CHUNK // slots + 3 * BLOCK * CHUNK // slots
    listed = send // LANES

    def kernel(*refs):
        place_ref = refs[len(given)]
        rows_ref, list_ref, sent_ref, table_w, hidden_w, out_w, node_pre = refs[len(given) + 1 :][:7]
        held = refs[len(given) + 8 :][: len(given)]
        wide, square, spread, arrived = refs[2 * len(given) + 8 :]
        copies = [
            pltpu.make_async_copy(source, target, arrived.at[at])
            for at, (source, target) in enumerate(zip(refs, held))
        ]
        for copy in copies:
            copy.start()
        for copy in copies:
            copy.wait()
        count_ref, nbr_ref, geom_ref, feat_ref, one_ref, hidden_ref, two_ref, out_ref, three_ref, send_ref = held
        member = place_ref[0]
        first_id = place_ref[2]
        start = place_ref[3]
        lane = lax.broadcasted_iota(jnp.int32, (1, LANES), 1)

        slot = lax.broadcasted_iota(jnp.int32, (1, slots), 1)
        rows_ref[...] = jnp.full((tall, slots), nothing, jnp.int32)
        together = 8

        def some_nodes(step, at):
            first = step * together
            counts = [count_ref[start + first + i] for i in range(together)]
            spots = []
            for i in range(together):
                spots.append(at)
                at = at + (counts[i] + CHUNK - 1) // CHUNK
            turned = []
            for i in range(together):
                row = nbr_ref[pl.ds(start + first + i, 1), :]
                row = jnp.where(row >= points + send, row - send, row)
                row = jnp.where(slot < counts[i], 2 * row, nothing)
                turned.append(pltpu.roll(row, (spots[i] % per_node) * CHUNK, 1))
            for i in range(together):
                line = spots[i] // per_node
                kept = slot < (spots[i] % per_node) * CHUNK
                rows_ref[pl.ds(line, 1), :] = jnp.where(kept, rows_ref[pl.ds(line, 1), :], turned[i])
                rows_ref[pl.ds(line + 1, 1), :] = turned[i]
                for piece in range(per_node):
                    list_ref[spots[i] + piece] = first + i
            return at

        used = lax.fori_loop(0, nodes // together, some_nodes, 0)

        def fill(step, carry):
            for i in range(8):
                list_ref[used + 8 * step + i] = nodes
            return carry

        lax.fori_loop(0, 3 * BLOCK // 8, fill, 0)
        list_ref[most + 3 * BLOCK] = (used + 2 * BLOCK - 1) // (2 * BLOCK)
        side = place_ref[1]
        chosen = send_ref[pl.ds(side, 1), :]
        for line in range(listed):
            sent_ref[line : line + 1, :] = chosen[:, line * LANES : (line + 1) * LANES]

        square[...] = jnp.zeros((LANES, LANES), jnp.float32)
        square[0:hidden, 0:channels] = feat_ref[...].astype(jnp.float32)
        square[...] = square[...].T
        wide[...] = jnp.zeros((LANES, 2 * LANES), jnp.float32)
        for block in range(groups):
            wide[block * width : block * width + chans, 0:LANES] = square[
                block * chans : (block + 1) * chans, :
            ]
        geom = geom_ref[...].astype(jnp.float32)
        wide[chans : chans + 3, 0:hidden] = geom[3:6]
        row = lax.broadcasted_iota(jnp.int32, (LANES, LANES), 0)
        col = lax.broadcasted_iota(jnp.int32, (LANES, LANES), 1)
        pair = member // 2
        take = ((row == pair * 2 * width + col) & (col < 2 * width)) | (
            (row == chans + 3) & (col == LANES - 1)
        )
        wide[:, LANES:] = take.astype(jnp.float32)
        table_w[...] = wide[...].astype(jnp.bfloat16)

        square[...] = jnp.zeros((LANES, LANES), jnp.float32)
        square[0:hidden, 0:hidden] = 0.5 * hidden_ref[...].astype(jnp.float32)
        square[...] = square[...].T
        square[extra, 0:hidden] = parts(two_ref[...])
        ones = (lane >= hidden) & (lane < hidden + 3)
        square[hidden : hidden + 1, hidden:] = jnp.where(ones, 0.5, 0.0)[:, hidden:]
        hidden_w[...] = square[...].astype(jnp.bfloat16)

        square[...] = jnp.zeros((LANES, LANES), jnp.float32)
        square[0:hidden, 0:channels] = 0.5 * out_ref[...].astype(jnp.float32)
        square[extra, 0:channels] = parts(three_ref[...])
        square[...] = square[...].T
        spread[...] = jnp.zeros((LANES, LANES), jnp.float32)
        for half in range(2):
            spread[half * width : half * width + chans, :] = square[
                pl.ds((2 * pair + half) * chans, chans), :
            ]
        spread[LANES - 1 :, :] = jnp.where(lane == hidden, 1.0 / CONSTANT, 0.0)
        out_w[...] = spread[...].T.astype(jnp.bfloat16)

        ids = first_id + lax.broadcasted_iota(jnp.int32, (nodes + 8, 1), 0)
        along_x = ((ids % GX).astype(jnp.float32) + 0.5) / GX
        along_y = ((ids // GX % GY).astype(jnp.float32) + 0.5) / GY
        along_z = ((ids // (GX * GY)).astype(jnp.float32) + 0.5) / depth
        term = geom[0:1] * along_x + geom[1:2] * along_y + geom[2:3] * along_z + one_ref[...]
        node_pre[...] = jnp.broadcast_to(jnp.where(ones, 0.5 * CONSTANT, 0.0), (nodes + 8, LANES))
        node_pre[:, 0:hidden] = term

    out = pl.pallas_call(
        kernel,
        out_shape=(
            jax.ShapeDtypeStruct((tall, slots), jnp.int32),
            jax.ShapeDtypeStruct((most + 3 * BLOCK + 1,), jnp.int32),
            jax.ShapeDtypeStruct((listed, LANES), jnp.int32),
            jax.ShapeDtypeStruct((LANES, 2 * LANES), jnp.bfloat16),
            jax.ShapeDtypeStruct((LANES, LANES), jnp.bfloat16),
            jax.ShapeDtypeStruct((LANES, LANES), jnp.bfloat16),
            jax.ShapeDtypeStruct((nodes + 8, LANES), jnp.float32),
        ),
        in_specs=[HBM] * len(given) + [SMEM],
        out_specs=(VMEM, SMEM, VMEM) + (VMEM,) * 4,
        scratch_shapes=[pltpu.SMEM(neighbour_count.shape, jnp.int32)]
        + [pltpu.VMEM(array.shape, array.dtype) for array in given[1:]]
        + [
            pltpu.VMEM((LANES, 2 * LANES), jnp.float32),
            pltpu.VMEM((LANES, LANES), jnp.float32),
            pltpu.VMEM((LANES, LANES), jnp.float32),
            pltpu.SemaphoreType.DMA((len(given),)),
        ],
        name="prepare",
    )(*given, place)
    return out[:2], out[2], out[3:]


def select_points(blocks, coords, send_rows, send_count, place):
    groups = len(blocks)
    chans, points = blocks[0].shape
    width = LANES // groups
    send = send_rows.shape[0] * LANES
    unroll = 16

    def kernel(*refs):
        block_refs = refs[:groups]
        coords_ref, rows_ref, count_ref, place_ref = refs[groups : groups + 4]
        own_ref, sent_ref, stack, table, picked = refs[groups + 4 :]
        member = place_ref[0]
        side = place_ref[1]
        for step in range(groups):
            base = pl.multiple_of((member ^ step) * width, width)
            empty = jnp.zeros((width - chans, points), jnp.bfloat16)
            stack[pl.ds(base, width), :] = jnp.concatenate([block_refs[step][...], empty], axis=0)
        stack[chans : chans + 3, :] = coords_ref[...]
        stack[chans + 3 : chans + 4, :] = jnp.ones((1, points), jnp.bfloat16)
        own = stack[...].T
        own_ref[...] = own
        table[...] = own.astype(jnp.float32)

        for base in range(0, send, unroll):
            rows = [
                table[pl.ds(rows_ref[at // LANES, at % LANES], 1), :] for at in range(base, base + unroll)
            ]
            for j in range(unroll):
                picked[base + j : base + j + 1, :] = rows[j]
        slot = lax.broadcasted_iota(jnp.int32, (send, LANES), 0)
        sent_ref[...] = jnp.where(slot < count_ref[side, 0], picked[...], 0.0).astype(jnp.bfloat16)

    return pl.pallas_call(
        kernel,
        out_shape=(
            jax.ShapeDtypeStruct((points, LANES), jnp.bfloat16),
            jax.ShapeDtypeStruct((send, LANES), jnp.bfloat16),
        ),
        in_specs=[VMEM] * (groups + 1) + [SMEM] * 3,
        out_specs=(VMEM, VMEM),
        scratch_shapes=[
            pltpu.VMEM((LANES, points), jnp.bfloat16),
            pltpu.VMEM((points, LANES), jnp.float32),
            pltpu.VMEM((send, LANES), jnp.float32),
        ],
        compiler_params=pltpu.CompilerParams(vmem_limit_bytes=12 << 20),
        name="select_points",
    )(*blocks, coords, send_rows, send_count, place)


def encode(own, other, plan, place, weights, chans, width):
    rows, spots = plan
    table_weight, hidden_weight, out_weight, node_part = weights
    points = own.shape[0]
    send = other.shape[0]
    nodes = node_part.shape[0] - 8
    slots = rows.shape[1]
    total_rows = points + send
    pairs = BLOCK * CHUNK
    lines = pairs // slots

    def kernel(
        own_ref, other_ref, rows_ref, spot_ref, place_ref, table_w, hidden_w, out_w, node_pre,
        keep_ref, give_ref, table, picked_a, picked_b, names_a, names_b, acc, turned, arrived,
    ):
        parity = place_ref[1]
        steps = spot_ref[spots.shape[0] - 1]

        def fetch(block, names, which):
            source = rows_ref.at[pl.ds(pl.multiple_of(block * lines, lines), lines), :]
            return pltpu.make_async_copy(source, names, arrived.at[which])

        fetch(0, names_a, 0).start()
        fetch(1, names_b, 1).start()

        def fill(source, start, count):
            step = 256
            for at in range(0, count, step):
                both = jnp.dot(source[pl.ds(at, step), :], table_w[...], preferred_element_type=jnp.float32)
                pre = both[:, :LANES].astype(jnp.bfloat16).astype(jnp.float32)
                table[pl.ds(2 * (start + at), step, stride=2), :] = pre
                table[pl.ds(2 * (start + at) + 1, step, stride=2), :] = both[:, LANES:]

        fill(own_ref, 0, points)
        fill(other_ref, points, send)
        table[pl.ds(2 * total_rows, 8), :] = jnp.zeros((8, LANES), jnp.float32)
        acc[...] = jnp.zeros((nodes + 8, 8, LANES), jnp.float32)

        def gather(names, picked):
            for base in range(0, pairs, CHUNK):
                got = [
                    table[pl.ds(names[at // slots, at % slots], 2), :] for at in range(base, base + CHUNK)
                ]
                for j in range(CHUNK):
                    picked[2 * (base + j) : 2 * (base + j) + 2, :] = got[j]

        def compute(block, picked):
            of_block = spot_ref.at[pl.ds(block * BLOCK, BLOCK)]
            step = 8
            for group in range(BLOCK // step):
                base = group * step * CHUNK
                here = [of_block[group * step + i] for i in range(step)]
                offset = jnp.concatenate(
                    [jnp.broadcast_to(node_pre[pl.ds(spot, 1), :], (CHUNK, LANES)) for spot in here],
                    axis=0,
                )
                pre = picked[pl.ds(2 * base, step * CHUNK, stride=2), :]
                val = picked[pl.ds(2 * base + 1, step * CHUNK, stride=2), :]
                first = gelu_doubled(pre + offset).astype(jnp.bfloat16)
                second = jnp.dot(first, hidden_w[...], preferred_element_type=jnp.float32)
                second = gelu_doubled(second).astype(jnp.bfloat16)
                kappa = jnp.dot(second, out_w[...], preferred_element_type=jnp.float32)
                product = kappa * val
                for i, spot in enumerate(here):
                    part = product[i * CHUNK : i * CHUNK + 8]
                    for j in range(8, CHUNK, 8):
                        part = part + product[i * CHUNK + j : i * CHUNK + j + 8]
                    acc[spot] = acc[spot] + part

        fetch(0, names_a, 0).wait()
        gather(names_a, picked_a)
        fetch(2, names_a, 0).start()

        def one_step(index, carry):
            block = 2 * index
            fetch(block + 1, names_b, 1).wait()
            gather(names_b, picked_b)
            compute(block, picked_a)
            fetch(block + 3, names_b, 1).start()
            fetch(block + 2, names_a, 0).wait()
            gather(names_a, picked_a)
            compute(block + 1, picked_b)
            fetch(block + 4, names_a, 0).start()
            return carry

        lax.fori_loop(0, steps, one_step, 0)
        fetch(0, names_a, 0).wait()
        fetch(1, names_b, 1).wait()
        sums = jnp.sum(acc[0:nodes], axis=1)
        means = (sums / sums[:, LANES - 1 :]).T
        low = jnp.where(parity == 1, means, 0.0)
        turned[...] = jnp.concatenate([low, means - low], axis=1)
        mine = pl.multiple_of((1 - parity) * width, width)
        theirs = pl.multiple_of(parity * width, width)
        keep_ref[...] = turned[pl.ds(mine, chans), :]
        give_ref[...] = turned[pl.ds(theirs, chans), :]

    piece = jax.ShapeDtypeStruct((chans, ZD * nodes), jnp.float32)
    return pl.pallas_call(
        kernel,
        out_shape=(piece, piece),
        in_specs=[VMEM, VMEM, VMEM, SMEM, SMEM] + [VMEM] * 4,
        out_specs=(VMEM, VMEM),
        scratch_shapes=[
            pltpu.VMEM((2 * total_rows + 8, LANES), jnp.float32),
            pltpu.VMEM((2 * pairs, LANES), jnp.float32),
            pltpu.VMEM((2 * pairs, LANES), jnp.float32),
            pltpu.SMEM((lines, slots), jnp.int32),
            pltpu.SMEM((lines, slots), jnp.int32),
            pltpu.VMEM((nodes + 8, 8, LANES), jnp.float32),
            pltpu.VMEM((LANES, ZD * nodes), jnp.float32),
            pltpu.SemaphoreType.DMA((2,)),
        ],
        compiler_params=pltpu.CompilerParams(vmem_limit_bytes=16 << 20),
        name="encode",
    )(own, other, rows, spots, place, table_weight, hidden_weight, out_weight, node_part)


def shards(
    features,
    coords,
    send_rows,
    send_count,
    neighbours,
    neighbour_count,
    geom_weight,
    feat_weight,
    bias_one,
    hidden_weight,
    bias_two,
    out_weight,
    bias_three,
):
    groups = lax.axis_size("chan")
    slabs = lax.axis_size("slab")
    member = lax.axis_index("chan")
    slab_id = lax.axis_index("slab")
    chans, points = features.shape
    per_slab = neighbours.shape[0]
    nodes = per_slab // ZD
    width = LANES // groups

    blocks = [features]
    for step in range(1, groups):
        blocks.append(lax.ppermute(features, "chan", [(i, i ^ step) for i in range(groups)]))

    plane = member % 2
    start = plane * nodes
    upper = 1 - plane
    place = jnp.stack([member, upper, slab_id * per_slab + start, start]).astype(jnp.int32)
    plan, sent_rows, weights = prepare(
        neighbours, neighbour_count, geom_weight, feat_weight, bias_one, hidden_weight, bias_two,
        out_weight, bias_three, place, groups, points, send_rows, ZD * slabs,
    )
    own, sent = select_points(blocks, coords, sent_rows, send_count, place)
    moves = []
    for slab in range(slabs):
        for who in range(groups):
            target = slab + 1 if who % 2 == 0 else slab - 1
            if 0 <= target < slabs:
                moves.append((slab * groups + who, target * groups + who))
    other = lax.ppermute(sent, ("slab", "chan"), moves)
    keep, give = encode(own, other, plan, place, weights, chans, width)
    return keep + lax.ppermute(give, "chan", [(i, i ^ 1) for i in range(groups)])


def solution(mesh):
    placed = (
        P("chan", "slab"),
        P(None, "slab"),
        P(None, "slab"),
        P(None, "slab"),
        P("slab", None),
        P("slab"),
        P(),
        P(),
        P(),
        P(),
        P(),
        P(),
        P(),
    )
    return jax.shard_map(
        shards, mesh=mesh, in_specs=placed, out_specs=P("chan", "slab"), check_vma=False
    )
```

```python
import jax
import jax.numpy as jnp
from jax import lax
from jax.experimental import pallas as pl
from jax.experimental.pallas import tpu as pltpu
from jax.sharding import PartitionSpec as P

ZD = 2
GX = 16
GY = 4
LANES = 128
CHUNK = 16
BLOCK = 64
CONSTANT = 16.0
GELU_ONE = 0.7978845608028654
GELU_CUBE = 0.044715 * GELU_ONE

SMEM = pl.BlockSpec(memory_space=pltpu.SMEM)
VMEM = pl.BlockSpec(memory_space=pltpu.VMEM)
HBM = pl.BlockSpec(memory_space=pltpu.MemorySpace.HBM)


def gelu_doubled(x):
    inner = x * (GELU_ONE + GELU_CUBE * (x * x))
    return x * (1.0 + jnp.tanh(inner))


def prepare(
    neighbours, neighbour_count, geom_weight, feat_weight, bias_one, hidden_weight, bias_two,
    out_weight, bias_three, groups, points, send_rows, depth,
):
    per_slab, slots = neighbours.shape
    send = send_rows.shape[1]
    hidden, channels = feat_weight.shape
    chans = channels // groups
    width = LANES // groups
    nodes = per_slab // ZD
    per_node = slots // CHUNK
    most = nodes * per_node
    nothing = 2 * (points + send)
    extra = slice(hidden, hidden + 3)

    def parts(value):
        high = value.astype(jnp.bfloat16).astype(jnp.float32)
        mid = (value - high).astype(jnp.bfloat16).astype(jnp.float32)
        low = (value - high - mid).astype(jnp.bfloat16).astype(jnp.float32)
        return jnp.concatenate([high, mid, low], axis=0) * (1.0 / CONSTANT)

    given = (
        neighbour_count, neighbours, geom_weight.T, feat_weight, bias_one[None], hidden_weight,
        bias_two[None], out_weight.T, bias_three[None], send_rows,
    )
    tall = most * CHUNK // slots + 3 * BLOCK * CHUNK // slots
    listed = send // LANES

    def kernel(*refs):
        rows_ref, spot_ref, sent_ref, table_w, hidden_w, out_w, node_pre = refs[len(given) :][:7]
        held = refs[len(given) + 7 :][: len(given)]
        wide, square, spread, arrived = refs[2 * len(given) + 7 :]
        copies = [
            pltpu.make_async_copy(source, target, arrived.at[at])
            for at, (source, target) in enumerate(zip(refs, held))
        ]
        for copy in copies:
            copy.start()
        for copy in copies:
            copy.wait()
        count_ref, nbr_ref, geom_ref, feat_ref, one_ref, hidden_ref, two_ref, out_ref, three_ref, send_ref = held
        member = lax.axis_index("chan")
        start = (member % ZD) * nodes
        first_id = lax.axis_index("slab") * per_slab + start
        lane = lax.broadcasted_iota(jnp.int32, (1, LANES), 1)

        slot = lax.broadcasted_iota(jnp.int32, (1, slots), 1)
        rows_ref[...] = jnp.full((tall, slots), nothing, jnp.int32)
        together = 8

        chunk = BLOCK * lax.broadcasted_iota(jnp.int32, (8, LANES), 0)
        chunk = chunk + lax.broadcasted_iota(jnp.int32, (8, LANES), 1)

        def some_nodes(step, carry):
            at, node_of = carry
            first = step * together
            counts = [count_ref[start + first + i] for i in range(together)]
            spots = []
            for i in range(together):
                spots.append(at)
                at = at + (counts[i] + CHUNK - 1) // CHUNK
            turned = []
            for i in range(together):
                row = nbr_ref[pl.ds(start + first + i, 1), :]
                row = jnp.where(row >= points + send, row - send, row)
                row = jnp.where(slot < counts[i], 2 * row, nothing)
                turned.append(pltpu.roll(row, (spots[i] % per_node) * CHUNK, 1))
            for i in range(together):
                line = spots[i] // per_node
                kept = slot < (spots[i] % per_node) * CHUNK
                rows_ref[pl.ds(line, 1), :] = jnp.where(kept, rows_ref[pl.ds(line, 1), :], turned[i])
                rows_ref[pl.ds(line + 1, 1), :] = turned[i]
            for end in spots[1:] + [at]:
                node_of = node_of + (chunk >= end).astype(jnp.int32)
            return at, node_of

        none = jnp.zeros((8, LANES), jnp.int32)
        used, node_of = lax.fori_loop(0, nodes // together, some_nodes, (jnp.int32(0), none))
        spot_ref[0:8, :] = node_of
        spot_ref[8:16, :] = none + (used + BLOCK - 1) // BLOCK
        side = 1 - member % ZD
        chosen = send_ref[pl.ds(side, 1), :]
        for line in range(listed):
            sent_ref[line : line + 1, :] = chosen[:, line * LANES : (line + 1) * LANES]

        square[...] = jnp.zeros((LANES, LANES), jnp.float32)
        square[0:hidden, 0:channels] = feat_ref[...].astype(jnp.float32)
        square[...] = square[...].T
        wide[...] = jnp.zeros((LANES, 2 * LANES), jnp.float32)
        for block in range(groups):
            wide[block * width : block * width + chans, 0:LANES] = square[
                block * chans : (block + 1) * chans, :
            ]
        geom = geom_ref[...].astype(jnp.float32)
        wide[chans : chans + 3, 0:hidden] = geom[3:6]
        row = lax.broadcasted_iota(jnp.int32, (LANES, LANES), 0)
        col = lax.broadcasted_iota(jnp.int32, (LANES, LANES), 1)
        pair = member // 2
        take = ((row == pair * 2 * width + col) & (col < 2 * width)) | (
            (row == chans + 3) & (col == LANES - 1)
        )
        wide[:, LANES:] = take.astype(jnp.float32)
        table_w[...] = wide[...].astype(jnp.bfloat16)

        square[...] = jnp.zeros((LANES, LANES), jnp.float32)
        square[0:hidden, 0:hidden] = 0.5 * hidden_ref[...].astype(jnp.float32)
        square[...] = square[...].T
        square[extra, 0:hidden] = parts(two_ref[...])
        ones = (lane >= hidden) & (lane < hidden + 3)
        square[hidden : hidden + 1, hidden:] = jnp.where(ones, 0.5, 0.0)[:, hidden:]
        hidden_w[...] = square[...].astype(jnp.bfloat16)

        square[...] = jnp.zeros((LANES, LANES), jnp.float32)
        square[0:hidden, 0:channels] = 0.5 * out_ref[...].astype(jnp.float32)
        square[extra, 0:channels] = parts(three_ref[...])
        square[...] = square[...].T
        spread[...] = jnp.zeros((LANES, LANES), jnp.float32)
        for half in range(2):
            spread[half * width : half * width + chans, :] = square[
                pl.ds((2 * pair + half) * chans, chans), :
            ]
        spread[LANES - 1 :, :] = jnp.where(lane == hidden, 1.0 / CONSTANT, 0.0)
        out_w[...] = spread[...].T.astype(jnp.bfloat16)

        ids = first_id + lax.broadcasted_iota(jnp.int32, (nodes + 8, 1), 0)
        along_x = ((ids % GX).astype(jnp.float32) + 0.5) / GX
        along_y = ((ids // GX % GY).astype(jnp.float32) + 0.5) / GY
        along_z = ((ids // (GX * GY)).astype(jnp.float32) + 0.5) / depth
        term = geom[0:1] * along_x + geom[1:2] * along_y + geom[2:3] * along_z + one_ref[...]
        node_pre[...] = jnp.broadcast_to(jnp.where(ones, 0.5 * CONSTANT, 0.0), (nodes + 8, LANES))
        node_pre[:, 0:hidden] = term

    out = pl.pallas_call(
        kernel,
        out_shape=(
            jax.ShapeDtypeStruct((tall, slots), jnp.int32),
            jax.ShapeDtypeStruct((16, LANES), jnp.int32),
            jax.ShapeDtypeStruct((listed, LANES), jnp.int32),
            jax.ShapeDtypeStruct((LANES, 2 * LANES), jnp.bfloat16),
            jax.ShapeDtypeStruct((LANES, LANES), jnp.bfloat16),
            jax.ShapeDtypeStruct((LANES, LANES), jnp.bfloat16),
            jax.ShapeDtypeStruct((nodes + 8, LANES), jnp.float32),
        ),
        in_specs=[HBM] * len(given),
        out_specs=(VMEM,) * 7,
        scratch_shapes=[pltpu.SMEM(neighbour_count.shape, jnp.int32)]
        + [pltpu.VMEM(array.shape, array.dtype) for array in given[1:]]
        + [
            pltpu.VMEM((LANES, 2 * LANES), jnp.float32),
            pltpu.VMEM((LANES, LANES), jnp.float32),
            pltpu.VMEM((LANES, LANES), jnp.float32),
            pltpu.SemaphoreType.DMA((len(given),)),
        ],
        name="prepare",
    )(*given)
    return out[:2], out[2], out[3:]


def select_points(blocks, coords, send_rows, send_count):
    groups = len(blocks)
    chans, points = blocks[0].shape
    width = LANES // groups
    send = send_rows.shape[0] * LANES
    unroll = 16

    def kernel(*refs):
        block_refs = refs[:groups]
        coords_ref, rows_ref, count_ref = refs[groups : groups + 3]
        own_ref, sent_ref, stack, table, picked = refs[groups + 3 :]
        member = lax.axis_index("chan")
        side = 1 - member % ZD
        for step in range(groups):
            base = pl.multiple_of((member ^ step) * width, width)
            empty = jnp.zeros((width - chans, points), jnp.bfloat16)
            stack[pl.ds(base, width), :] = jnp.concatenate([block_refs[step][...], empty], axis=0)
        stack[chans : chans + 3, :] = coords_ref[...]
        stack[chans + 3 : chans + 4, :] = jnp.ones((1, points), jnp.bfloat16)
        own = stack[...].T
        own_ref[...] = own
        table[...] = own.astype(jnp.float32)

        for base in range(0, send, unroll):
            rows = [
                table[pl.ds(rows_ref[at // LANES, at % LANES], 1), :] for at in range(base, base + unroll)
            ]
            for j in range(unroll):
                picked[base + j : base + j + 1, :] = rows[j]
        slot = lax.broadcasted_iota(jnp.int32, (send, LANES), 0)
        sent_ref[...] = jnp.where(slot < count_ref[side, 0], picked[...], 0.0).astype(jnp.bfloat16)

    return pl.pallas_call(
        kernel,
        out_shape=(
            jax.ShapeDtypeStruct((points, LANES), jnp.bfloat16),
            jax.ShapeDtypeStruct((send, LANES), jnp.bfloat16),
        ),
        in_specs=[VMEM] * (groups + 1) + [SMEM] * 2,
        out_specs=(VMEM, VMEM),
        scratch_shapes=[
            pltpu.VMEM((LANES, points), jnp.bfloat16),
            pltpu.VMEM((points, LANES), jnp.float32),
            pltpu.VMEM((send, LANES), jnp.float32),
        ],
        compiler_params=pltpu.CompilerParams(vmem_limit_bytes=12 << 20),
        name="select_points",
    )(*blocks, coords, send_rows, send_count)


def encode(own, other, plan, weights, chans, width):
    rows, spots = plan
    table_weight, hidden_weight, out_weight, node_part = weights
    points = own.shape[0]
    send = other.shape[0]
    nodes = node_part.shape[0] - 8
    slots = rows.shape[1]
    total_rows = points + send
    pairs = BLOCK * CHUNK
    lines = pairs // slots

    def kernel(
        own_ref, other_ref, rows_ref, spots_ref, table_w, hidden_w, out_w, node_pre,
        keep_ref, give_ref, table, picked, names_a, names_b, spot_ref, acc, turned,
        arrived,
    ):
        parity = 1 - lax.axis_index("chan") % ZD

        def fetch(block, names, which):
            source = rows_ref.at[pl.ds(pl.multiple_of(block * lines, lines), lines), :]
            return pltpu.make_async_copy(source, names, arrived.at[which])

        fetch(0, names_a, 0).start()
        fetch(1, names_b, 1).start()
        of_blocks = pltpu.make_async_copy(spots_ref, spot_ref, arrived.at[2])
        of_blocks.start()

        def fill(source, start, count):
            step = 256
            for at in range(0, count, step):
                both = jnp.dot(source[pl.ds(at, step), :], table_w[...], preferred_element_type=jnp.float32)
                pre = both[:, :LANES].astype(jnp.bfloat16).astype(jnp.float32)
                table[pl.ds(2 * (start + at), step, stride=2), :] = pre
                table[pl.ds(2 * (start + at) + 1, step, stride=2), :] = both[:, LANES:]

        fill(own_ref, 0, points)
        fill(other_ref, points, send)
        table[pl.ds(2 * total_rows, 8), :] = jnp.zeros((8, LANES), jnp.float32)
        acc[...] = jnp.zeros((nodes + 8, 8, LANES), jnp.float32)

        def one_block(block, names):
            for base in range(0, pairs, CHUNK):
                got = [
                    table[pl.ds(names[at // slots, at % slots], 2), :] for at in range(base, base + CHUNK)
                ]
                for j in range(CHUNK):
                    picked[2 * (base + j) : 2 * (base + j) + 2, :] = got[j]
            step = 8
            for group in range(BLOCK // step):
                base = group * step * CHUNK
                here = [spot_ref[block, group * step + i] for i in range(step)]
                offset = jnp.concatenate(
                    [jnp.broadcast_to(node_pre[pl.ds(spot, 1), :], (CHUNK, LANES)) for spot in here],
                    axis=0,
                )
                pre = picked[pl.ds(2 * base, step * CHUNK, stride=2), :]
                val = picked[pl.ds(2 * base + 1, step * CHUNK, stride=2), :]
                first = gelu_doubled(pre + offset).astype(jnp.bfloat16)
                second = jnp.dot(first, hidden_w[...], preferred_element_type=jnp.float32)
                second = gelu_doubled(second).astype(jnp.bfloat16)
                kappa = jnp.dot(second, out_w[...], preferred_element_type=jnp.float32)
                product = kappa * val
                for i, spot in enumerate(here):
                    part = product[i * CHUNK : i * CHUNK + 8]
                    for j in range(8, CHUNK, 8):
                        part = part + product[i * CHUNK + j : i * CHUNK + j + 8]
                    acc[spot] = acc[spot] + part

        def one_step(index, carry):
            block = 2 * index
            fetch(block, names_a, 0).wait()
            one_block(block, names_a)
            fetch(block + 2, names_a, 0).start()
            fetch(block + 1, names_b, 1).wait()

            @pl.when(block + 1 < spot_ref[spots.shape[0] - 1, 0])
            def _():
                one_block(block + 1, names_b)

            fetch(block + 3, names_b, 1).start()
            return carry

        of_blocks.wait()
        blocks = spot_ref[spots.shape[0] - 1, 0]
        lax.fori_loop(0, (blocks + 1) // 2, one_step, 0)
        fetch(0, names_a, 0).wait()
        fetch(1, names_b, 1).wait()
        sums = jnp.sum(acc[0:nodes], axis=1)
        means = (sums / sums[:, LANES - 1 :]).T
        low = jnp.where(parity == 1, means, 0.0)
        turned[...] = jnp.concatenate([low, means - low], axis=1)
        mine = pl.multiple_of((1 - parity) * width, width)
        theirs = pl.multiple_of(parity * width, width)
        keep_ref[...] = turned[pl.ds(mine, chans), :]
        give_ref[...] = turned[pl.ds(theirs, chans), :]

    piece = jax.ShapeDtypeStruct((chans, ZD * nodes), jnp.float32)
    return pl.pallas_call(
        kernel,
        out_shape=(piece, piece),
        in_specs=[VMEM] * 8,
        out_specs=(VMEM, VMEM),
        scratch_shapes=[
            pltpu.VMEM((2 * total_rows + 8, LANES), jnp.float32),
            pltpu.VMEM((2 * pairs, LANES), jnp.float32),
            pltpu.SMEM((lines, slots), jnp.int32),
            pltpu.SMEM((lines, slots), jnp.int32),
            pltpu.SMEM(spots.shape, jnp.int32),
            pltpu.VMEM((nodes + 8, 8, LANES), jnp.float32),
            pltpu.VMEM((LANES, ZD * nodes), jnp.float32),
            pltpu.SemaphoreType.DMA((3,)),
        ],
        compiler_params=pltpu.CompilerParams(vmem_limit_bytes=16 << 20),
        name="encode",
    )(own, other, rows, spots, table_weight, hidden_weight, out_weight, node_part)


def shards(
    features,
    coords,
    send_rows,
    send_count,
    neighbours,
    neighbour_count,
    geom_weight,
    feat_weight,
    bias_one,
    hidden_weight,
    bias_two,
    out_weight,
    bias_three,
):
    groups = lax.axis_size("chan")
    slabs = lax.axis_size("slab")
    chans, points = features.shape
    width = LANES // groups

    blocks = [features]
    for step in range(1, groups):
        blocks.append(lax.ppermute(features, "chan", [(i, i ^ step) for i in range(groups)]))

    plan, sent_rows, weights = prepare(
        neighbours, neighbour_count, geom_weight, feat_weight, bias_one, hidden_weight, bias_two,
        out_weight, bias_three, groups, points, send_rows, ZD * slabs,
    )
    own, sent = select_points(blocks, coords, sent_rows, send_count)
    moves = []
    for slab in range(slabs):
        for who in range(groups):
            target = slab + 1 if who % 2 == 0 else slab - 1
            if 0 <= target < slabs:
                moves.append((slab * groups + who, target * groups + who))
    other = lax.ppermute(sent, ("slab", "chan"), moves)
    keep, give = encode(own, other, plan, weights, chans, width)
    return keep + lax.ppermute(give, "chan", [(i, i ^ 1) for i in range(groups)])


def solution(mesh):
    placed = (
        P("chan", "slab"),
        P(None, "slab"),
        P(None, "slab"),
        P(None, "slab"),
        P("slab", None),
        P("slab"),
        P(),
        P(),
        P(),
        P(),
        P(),
        P(),
        P(),
    )
    return jax.shard_map(
        shards, mesh=mesh, in_specs=placed, out_specs=P("chan", "slab"), check_vma=False
    )
```

```python
import jax
import jax.numpy as jnp
from jax import lax
from jax.experimental import pallas as pl
from jax.experimental.pallas import tpu as pltpu
from jax.sharding import PartitionSpec as P


ZD = 2
GX = 16
GY = 4
LANES = 128
CHUNK = 16
BLOCK = 64
CONSTANT = 16.0
GELU_ONE = 0.7978845608028654
GELU_CUBE = 0.044715 * GELU_ONE

SMEM = pl.BlockSpec(memory_space=pltpu.SMEM)
VMEM = pl.BlockSpec(memory_space=pltpu.VMEM)
HBM = pl.BlockSpec(memory_space=pltpu.MemorySpace.HBM)


def gelu_doubled(x):
    inner = x * (GELU_ONE + GELU_CUBE * (x * x))
    return x * (1.0 + jnp.tanh(inner))


def prepare(
    neighbours, neighbour_count, geom_weight, feat_weight, bias_one, hidden_weight, bias_two,
    out_weight, bias_three, groups, points, send_rows, depth,
):
    per_slab, slots = neighbours.shape
    send = send_rows.shape[1]
    hidden, channels = feat_weight.shape
    chans = channels // groups
    width = LANES // groups
    nodes = per_slab // ZD
    per_node = slots // CHUNK
    most = nodes * per_node
    nothing = 2 * (points + send)
    extra = slice(hidden, hidden + 3)

    def parts(value):
        high = value.astype(jnp.bfloat16).astype(jnp.float32)
        mid = (value - high).astype(jnp.bfloat16).astype(jnp.float32)
        low = (value - high - mid).astype(jnp.bfloat16).astype(jnp.float32)
        return jnp.concatenate([high, mid, low], axis=0) * (1.0 / CONSTANT)

    given = (
        neighbour_count, neighbours, geom_weight.T, feat_weight, bias_one[None], hidden_weight,
        bias_two[None], out_weight.T, bias_three[None], send_rows,
    )
    tall = most * CHUNK // slots + 3 * BLOCK * CHUNK // slots
    listed = send // LANES

    def kernel(*refs):
        rows_ref, spot_ref, sent_ref, table_w, hidden_w, out_w, node_pre = refs[len(given) :][:7]
        held = refs[len(given) + 7 :][: len(given)]
        wide, square, spread, arrived = refs[2 * len(given) + 7 :]
        copies = [
            pltpu.make_async_copy(source, target, arrived.at[at])
            for at, (source, target) in enumerate(zip(refs, held))
        ]
        for copy in copies:
            copy.start()
        for copy in copies:
            copy.wait()
        count_ref, nbr_ref, geom_ref, feat_ref, one_ref, hidden_ref, two_ref, out_ref, three_ref, send_ref = held
        member = lax.axis_index("chan")
        start = (member % ZD) * nodes
        first_id = lax.axis_index("slab") * per_slab + start
        lane = lax.broadcasted_iota(jnp.int32, (1, LANES), 1)

        slot = lax.broadcasted_iota(jnp.int32, (1, slots), 1)
        rows_ref[...] = jnp.full((tall, slots), nothing, jnp.int32)
        together = 8

        chunk = BLOCK * lax.broadcasted_iota(jnp.int32, (8, LANES), 0)
        chunk = chunk + lax.broadcasted_iota(jnp.int32, (8, LANES), 1)

        def some_nodes(step, carry):
            at, node_of = carry
            first = step * together
            counts = [count_ref[start + first + i] for i in range(together)]
            spots = []
            for i in range(together):
                spots.append(at)
                at = at + (counts[i] + CHUNK - 1) // CHUNK
            turned = []
            for i in range(together):
                row = nbr_ref[pl.ds(start + first + i, 1), :]
                row = jnp.where(row >= points + send, row - send, row)
                row = jnp.where(slot < counts[i], 2 * row, nothing)
                turned.append(pltpu.roll(row, (spots[i] % per_node) * CHUNK, 1))
            for i in range(together):
                line = spots[i] // per_node
                kept = slot < (spots[i] % per_node) * CHUNK
                rows_ref[pl.ds(line, 1), :] = jnp.where(kept, rows_ref[pl.ds(line, 1), :], turned[i])
                rows_ref[pl.ds(line + 1, 1), :] = turned[i]
            for end in spots[1:] + [at]:
                node_of = node_of + (chunk >= end).astype(jnp.int32)
            return at, node_of

        none = jnp.zeros((8, LANES), jnp.int32)
        used, node_of = lax.fori_loop(0, nodes // together, some_nodes, (jnp.int32(0), none))
        spot_ref[0:8, :] = node_of
        spot_ref[8:16, :] = none + (used + BLOCK - 1) // BLOCK
        side = 1 - member % ZD
        chosen = send_ref[pl.ds(side, 1), :]
        for line in range(listed):
            sent_ref[line : line + 1, :] = chosen[:, line * LANES : (line + 1) * LANES]

        square[...] = jnp.zeros((LANES, LANES), jnp.float32)
        square[0:hidden, 0:channels] = feat_ref[...].astype(jnp.float32)
        square[...] = square[...].T
        wide[...] = jnp.zeros((LANES, 2 * LANES), jnp.float32)
        for block in range(groups):
            wide[block * width : block * width + chans, 0:LANES] = square[
                block * chans : (block + 1) * chans, :
            ]
        geom = geom_ref[...].astype(jnp.float32)
        wide[chans : chans + 3, 0:hidden] = geom[3:6]
        row = lax.broadcasted_iota(jnp.int32, (LANES, LANES), 0)
        col = lax.broadcasted_iota(jnp.int32, (LANES, LANES), 1)
        pair = member // 2
        take = ((row == pair * 2 * width + col) & (col < 2 * width)) | (
            (row == chans + 3) & (col == LANES - 1)
        )
        wide[:, LANES:] = take.astype(jnp.float32)
        table_w[...] = wide[...].astype(jnp.bfloat16)

        square[...] = jnp.zeros((LANES, LANES), jnp.float32)
        square[0:hidden, 0:hidden] = 0.5 * hidden_ref[...].astype(jnp.float32)
        square[...] = square[...].T
        square[extra, 0:hidden] = parts(two_ref[...])
        ones = (lane >= hidden) & (lane < hidden + 3)
        square[hidden : hidden + 1, hidden:] = jnp.where(ones, 0.5, 0.0)[:, hidden:]
        hidden_w[...] = square[...].astype(jnp.bfloat16)

        square[...] = jnp.zeros((LANES, LANES), jnp.float32)
        square[0:hidden, 0:channels] = 0.5 * out_ref[...].astype(jnp.float32)
        square[extra, 0:channels] = parts(three_ref[...])
        square[...] = square[...].T
        spread[...] = jnp.zeros((LANES, LANES), jnp.float32)
        for half in range(2):
            spread[half * width : half * width + chans, :] = square[
                pl.ds((2 * pair + half) * chans, chans), :
            ]
        spread[LANES - 1 :, :] = jnp.where(lane == hidden, 1.0 / CONSTANT, 0.0)
        out_w[...] = spread[...].T.astype(jnp.bfloat16)

        ids = first_id + lax.broadcasted_iota(jnp.int32, (nodes + 8, 1), 0)
        along_x = ((ids % GX).astype(jnp.float32) + 0.5) / GX
        along_y = ((ids // GX % GY).astype(jnp.float32) + 0.5) / GY
        along_z = ((ids // (GX * GY)).astype(jnp.float32) + 0.5) / depth
        term = geom[0:1] * along_x + geom[1:2] * along_y + geom[2:3] * along_z + one_ref[...]
        node_pre[...] = jnp.broadcast_to(jnp.where(ones, 0.5 * CONSTANT, 0.0), (nodes + 8, LANES))
        node_pre[:, 0:hidden] = term

    out = pl.pallas_call(
        kernel,
        out_shape=(
            jax.ShapeDtypeStruct((tall, slots), jnp.int32),
            jax.ShapeDtypeStruct((16, LANES), jnp.int32),
            jax.ShapeDtypeStruct((listed, LANES), jnp.int32),
            jax.ShapeDtypeStruct((LANES, 2 * LANES), jnp.bfloat16),
            jax.ShapeDtypeStruct((LANES, LANES), jnp.bfloat16),
            jax.ShapeDtypeStruct((LANES, LANES), jnp.bfloat16),
            jax.ShapeDtypeStruct((nodes + 8, LANES), jnp.float32),
        ),
        in_specs=[HBM] * len(given),
        out_specs=(VMEM,) * 7,
        scratch_shapes=[pltpu.SMEM(neighbour_count.shape, jnp.int32)]
        + [pltpu.VMEM(array.shape, array.dtype) for array in given[1:]]
        + [
            pltpu.VMEM((LANES, 2 * LANES), jnp.float32),
            pltpu.VMEM((LANES, LANES), jnp.float32),
            pltpu.VMEM((LANES, LANES), jnp.float32),
            pltpu.SemaphoreType.DMA((len(given),)),
        ],
        name="prepare",
    )(*given)
    return out[:2], out[2], out[3:]


def select_points(blocks, first_step, coords, sent_rows, send_count, groups, earlier=None):
    chans, points = blocks[0].shape
    width = LANES // groups
    send = sent_rows.shape[0] * LANES
    unroll = 16
    late = earlier is not None
    extra = (earlier,) if late else (coords,)

    def kernel(*refs):
        block_refs = refs[: len(blocks)]
        extra_ref, list_ref, count_ref, own_ref, sent_ref = refs[len(blocks) :][:5]
        stack, table, picked, rows_ref, arrived = refs[len(blocks) + 5 :][:5]
        listed = pltpu.make_async_copy(list_ref, rows_ref, arrived)
        listed.start()
        member = lax.axis_index("chan")
        side = 1 - member % ZD
        empty = jnp.zeros((width - chans, points), jnp.bfloat16)
        known = range(first_step, first_step + len(blocks))
        for step in range(groups):
            base = pl.multiple_of((member ^ step) * width, width)
            if step in known:
                block = jnp.concatenate([block_refs[step - first_step][...], empty], axis=0)
            else:
                block = jnp.zeros((width, points), jnp.bfloat16)
            stack[pl.ds(base, width), :] = block
        if not late:
            stack[chans : chans + 3, :] = extra_ref[...]
            stack[chans + 3 : chans + 4, :] = jnp.ones((1, points), jnp.bfloat16)
        own = stack[...].T
        own_ref[...] = own + extra_ref[...] if late else own
        table[...] = own.astype(jnp.float32)
        listed.wait()
        for base in range(0, send, unroll):
            rows = [
                table[pl.ds(rows_ref[at // LANES, at % LANES], 1), :] for at in range(base, base + unroll)
            ]
            for j in range(unroll):
                picked[base + j : base + j + 1, :] = rows[j]
        slot = lax.broadcasted_iota(jnp.int32, (send, LANES), 0)
        live = jnp.where(slot < count_ref[0, side], picked[...], 0.0)
        if late:
            turned = refs[-1]
            turned[...] = live.T
            base = pl.multiple_of((member ^ first_step) * width, width)
            sent_ref[...] = turned[pl.ds(base, width), :].astype(jnp.bfloat16)
        else:
            sent_ref[...] = live.astype(jnp.bfloat16)

    return pl.pallas_call(
        kernel,
        out_shape=(
            jax.ShapeDtypeStruct((points, LANES), jnp.bfloat16),
            jax.ShapeDtypeStruct((width, send) if late else (send, LANES), jnp.bfloat16),
        ),
        in_specs=[VMEM] * (len(blocks) + 1) + [HBM, SMEM],
        out_specs=(VMEM, VMEM),
        scratch_shapes=[
            pltpu.VMEM((LANES, points), jnp.bfloat16),
            pltpu.VMEM((points, LANES), jnp.float32),
            pltpu.VMEM((send, LANES), jnp.float32),
            pltpu.SMEM(sent_rows.shape, jnp.int32),
            pltpu.SemaphoreType.DMA,
        ]
        + [pltpu.VMEM((LANES, send), jnp.float32)] * late,
        compiler_params=pltpu.CompilerParams(vmem_limit_bytes=12 << 20),
        name="select_late" if late else "select_points",
    )(*blocks, *extra, sent_rows, send_count)


def encode(own, other, other_late, plan, weights, chans, width, groups):
    rows, spots = plan
    table_weight, hidden_weight, out_weight, node_part = weights
    points = own.shape[0]
    send = other.shape[0]
    nodes = node_part.shape[0] - 8
    slots = rows.shape[1]
    total_rows = points + send
    pairs = BLOCK * CHUNK
    lines = pairs // slots

    def kernel(
        own_ref, other_ref, late_ref, rows_ref, spots_ref, table_w, hidden_w, out_w, node_pre,
        keep_ref, give_ref, table, picked, names_a, names_b, spot_ref, acc, turned,
        late, whole, arrived,
    ):
        parity = 1 - lax.axis_index("chan") % ZD

        def fetch(block, names, which):
            source = rows_ref.at[pl.ds(pl.multiple_of(block * lines, lines), lines), :]
            return pltpu.make_async_copy(source, names, arrived.at[which])

        fetch(0, names_a, 0).start()
        fetch(1, names_b, 1).start()
        of_blocks = pltpu.make_async_copy(spots_ref, spot_ref, arrived.at[2])
        of_blocks.start()

        def fill(source, start, count):
            step = 256
            for at in range(0, count, step):
                both = jnp.dot(source[pl.ds(at, step), :], table_w[...], preferred_element_type=jnp.float32)
                pre = both[:, :LANES].astype(jnp.bfloat16).astype(jnp.float32)
                table[pl.ds(2 * (start + at), step, stride=2), :] = pre
                table[pl.ds(2 * (start + at) + 1, step, stride=2), :] = both[:, LANES:]

        fill(own_ref, 0, points)
        base = pl.multiple_of((lax.axis_index("chan") ^ (groups - 1)) * width, width)
        late[...] = jnp.zeros((LANES, send), jnp.bfloat16)
        late[pl.ds(base, width), :] = late_ref[...]
        whole[...] = other_ref[...] + late[...].T
        fill(whole, points, send)
        table[pl.ds(2 * total_rows, 8), :] = jnp.zeros((8, LANES), jnp.float32)
        acc[...] = jnp.zeros((nodes + 8, 8, LANES), jnp.float32)

        def one_block(block, names):
            for base in range(0, pairs, CHUNK):
                got = [
                    table[pl.ds(names[at // slots, at % slots], 2), :] for at in range(base, base + CHUNK)
                ]
                for j in range(CHUNK):
                    picked[2 * (base + j) : 2 * (base + j) + 2, :] = got[j]
            step = 8
            for group in range(BLOCK // step):
                base = group * step * CHUNK
                here = [spot_ref[block, group * step + i] for i in range(step)]
                offset = jnp.concatenate(
                    [jnp.broadcast_to(node_pre[pl.ds(spot, 1), :], (CHUNK, LANES)) for spot in here],
                    axis=0,
                )
                pre = picked[pl.ds(2 * base, step * CHUNK, stride=2), :]
                val = picked[pl.ds(2 * base + 1, step * CHUNK, stride=2), :]
                first = gelu_doubled(pre + offset).astype(jnp.bfloat16)
                second = jnp.dot(first, hidden_w[...], preferred_element_type=jnp.float32)
                second = gelu_doubled(second).astype(jnp.bfloat16)
                kappa = jnp.dot(second, out_w[...], preferred_element_type=jnp.float32)
                product = kappa * val
                for i, spot in enumerate(here):
                    part = product[i * CHUNK : i * CHUNK + 8]
                    for j in range(8, CHUNK, 8):
                        part = part + product[i * CHUNK + j : i * CHUNK + j + 8]
                    acc[spot] = acc[spot] + part

        def one_step(index, carry):
            block = 2 * index
            fetch(block, names_a, 0).wait()
            one_block(block, names_a)
            fetch(block + 2, names_a, 0).start()
            fetch(block + 1, names_b, 1).wait()

            @pl.when(block + 1 < spot_ref[spots.shape[0] - 1, 0])
            def _():
                one_block(block + 1, names_b)

            fetch(block + 3, names_b, 1).start()
            return carry

        of_blocks.wait()
        blocks = spot_ref[spots.shape[0] - 1, 0]
        lax.fori_loop(0, (blocks + 1) // 2, one_step, 0)
        fetch(0, names_a, 0).wait()
        fetch(1, names_b, 1).wait()
        sums = jnp.sum(acc[0:nodes], axis=1)
        means = (sums / sums[:, LANES - 1 :]).T
        low = jnp.where(parity == 1, means, 0.0)
        turned[...] = jnp.concatenate([low, means - low], axis=1)
        mine = pl.multiple_of((1 - parity) * width, width)
        theirs = pl.multiple_of(parity * width, width)
        keep_ref[...] = turned[pl.ds(mine, chans), :]
        give_ref[...] = turned[pl.ds(theirs, chans), :]

    piece = jax.ShapeDtypeStruct((chans, ZD * nodes), jnp.float32)
    return pl.pallas_call(
        kernel,
        out_shape=(piece, piece),
        in_specs=[VMEM] * 9,
        out_specs=(VMEM, VMEM),
        scratch_shapes=[
            pltpu.VMEM((2 * total_rows + 8, LANES), jnp.float32),
            pltpu.VMEM((2 * pairs, LANES), jnp.float32),
            pltpu.SMEM((lines, slots), jnp.int32),
            pltpu.SMEM((lines, slots), jnp.int32),
            pltpu.SMEM(spots.shape, jnp.int32),
            pltpu.VMEM((nodes + 8, 8, LANES), jnp.float32),
            pltpu.VMEM((LANES, ZD * nodes), jnp.float32),
            pltpu.VMEM((LANES, send), jnp.bfloat16),
            pltpu.VMEM((send, LANES), jnp.bfloat16),
            pltpu.SemaphoreType.DMA((3,)),
        ],
        compiler_params=pltpu.CompilerParams(vmem_limit_bytes=16 << 20),
        name="encode",
    )(own, other, other_late, rows, spots, table_weight, hidden_weight, out_weight, node_part)


def shards(
    features,
    coords,
    send_rows,
    send_count,
    neighbours,
    neighbour_count,
    geom_weight,
    feat_weight,
    bias_one,
    hidden_weight,
    bias_two,
    out_weight,
    bias_three,
):
    groups = lax.axis_size("chan")
    slabs = lax.axis_size("slab")
    chans, points = features.shape
    width = LANES // groups

    blocks = [features]
    for step in range(1, groups):
        blocks.append(lax.ppermute(features, "chan", [(i, i ^ step) for i in range(groups)]))

    plan, sent_rows, weights = prepare(
        neighbours, neighbour_count, geom_weight, feat_weight, bias_one, hidden_weight, bias_two,
        out_weight, bias_three, groups, points, send_rows, ZD * slabs,
    )

    early, sent = select_points(blocks[:-1], 0, coords, sent_rows, send_count.T, groups)
    moves = []
    for slab in range(slabs):
        for who in range(groups):
            target = slab + 1 if who % 2 == 0 else slab - 1
            if 0 <= target < slabs:
                moves.append((slab * groups + who, target * groups + who))
    other = lax.ppermute(sent, ("slab", "chan"), moves)
    own, sent_late = select_points(
        blocks[-1:], groups - 1, None, sent_rows, send_count.T, groups, early
    )
    other_late = lax.ppermute(sent_late, ("slab", "chan"), moves)
    keep, give = encode(own, other, other_late, plan, weights, chans, width, groups)
    return keep + lax.ppermute(give, "chan", [(i, i ^ 1) for i in range(groups)])


def solution(mesh):
    placed = (
        P("chan", "slab"),
        P(None, "slab"),
        P(None, "slab"),
        P(None, "slab"),
        P("slab", None),
        P("slab"),
        P(),
        P(),
        P(),
        P(),
        P(),
        P(),
        P(),
    )
    return jax.shard_map(
        shards, mesh=mesh, in_specs=placed, out_specs=P("chan", "slab"), check_vma=False
    )
```

```python
import jax
import jax.numpy as jnp
from jax import lax
from jax.experimental import pallas as pl
from jax.experimental.pallas import tpu as pltpu
from jax.sharding import PartitionSpec as P

ZD = 2
GX = 16
GY = 4
LANES = 128
CHUNK = 16
BLOCK = 64
GELU_ONE = 0.7978845608028654
GELU_CUBE = 0.044715 * GELU_ONE

SMEM = pl.BlockSpec(memory_space=pltpu.SMEM)
VMEM = pl.BlockSpec(memory_space=pltpu.VMEM)
HBM = pl.BlockSpec(memory_space=pltpu.MemorySpace.HBM)


def gelu_doubled(x):
    inner = x * (GELU_ONE + GELU_CUBE * (x * x))
    return x * (1.0 + jnp.tanh(inner))


def prepare(
    neighbours, neighbour_count, geom_weight, feat_weight, bias_one, hidden_weight, bias_two,
    out_weight, bias_three, groups, points, send_rows, depth,
):
    per_slab, slots = neighbours.shape
    send = send_rows.shape[1]
    hidden, channels = feat_weight.shape
    chans = channels // groups
    width = LANES // groups
    nodes = per_slab // ZD
    per_node = slots // CHUNK
    most = nodes * per_node
    nothing = points + send

    given = (
        neighbour_count, neighbours, geom_weight.T, feat_weight, bias_one[None], hidden_weight,
        bias_two[None], out_weight.T, bias_three[None], send_rows,
    )
    tall = most * CHUNK // slots + 3 * BLOCK * CHUNK // slots
    listed = send // LANES

    def kernel(*refs):
        rows_ref, spot_ref, sent_ref, halo_ref, table_w, hidden_w, out_w, node_pre, vec_ref = refs[
            len(given) :
        ][:9]
        held = refs[len(given) + 9 :][: len(given)]
        wide, square, spread, arrived = refs[2 * len(given) + 9 :]
        copies = [
            pltpu.make_async_copy(source, target, arrived.at[at])
            for at, (source, target) in enumerate(zip(refs, held))
        ]
        for copy in copies:
            copy.start()
        for copy in copies:
            copy.wait()
        count_ref, nbr_ref, geom_ref, feat_ref, one_ref, hidden_ref, two_ref, out_ref, three_ref, send_ref = held
        member = lax.axis_index("chan")
        start = (member % ZD) * nodes
        first_id = lax.axis_index("slab") * per_slab + start

        slot = lax.broadcasted_iota(jnp.int32, (1, slots), 1)
        rows_ref[...] = jnp.full((tall, slots), nothing, jnp.int32)
        together = 8

        chunk = BLOCK * lax.broadcasted_iota(jnp.int32, (8, LANES), 0)
        chunk = chunk + lax.broadcasted_iota(jnp.int32, (8, LANES), 1)

        def some_nodes(step, carry):
            at, node_of = carry
            first = step * together
            counts = [count_ref[start + first + i] for i in range(together)]
            spots = []
            for i in range(together):
                spots.append(at)
                at = at + (counts[i] + CHUNK - 1) // CHUNK
            turned = []
            for i in range(together):
                row = nbr_ref[pl.ds(start + first + i, 1), :]
                row = jnp.where(row >= points + send, row - send, row)
                row = jnp.where(slot < counts[i], row, nothing)
                halo = jnp.where(row < points, -1, row - points).astype(jnp.float32)
                halo_ref[pl.ds(first + i, 1), :] = halo
                turned.append(pltpu.roll(row, (spots[i] % per_node) * CHUNK, 1))
            for i in range(together):
                line = spots[i] // per_node
                kept = slot < (spots[i] % per_node) * CHUNK
                rows_ref[pl.ds(line, 1), :] = jnp.where(kept, rows_ref[pl.ds(line, 1), :], turned[i])
                rows_ref[pl.ds(line + 1, 1), :] = turned[i]
            for end in spots[1:] + [at]:
                node_of = node_of + (chunk >= end).astype(jnp.int32)
            return at, node_of

        none = jnp.zeros((8, LANES), jnp.int32)
        used, node_of = lax.fori_loop(0, nodes // together, some_nodes, (jnp.int32(0), none))
        spot_ref[0:8, :] = node_of
        spot_ref[8:16, :] = none + (used + BLOCK - 1) // BLOCK
        side = 1 - member % ZD
        chosen = send_ref[pl.ds(side, 1), :]
        for line in range(listed):
            sent_ref[line : line + 1, :] = chosen[:, line * LANES : (line + 1) * LANES]

        square[...] = jnp.zeros((LANES, LANES), jnp.float32)
        square[0:hidden, 0:channels] = feat_ref[...].astype(jnp.float32)
        square[...] = square[...].T
        wide[...] = jnp.zeros((LANES, LANES), jnp.float32)
        for block in range(groups):
            wide[block * width : block * width + chans, :] = square[
                block * chans : (block + 1) * chans, :
            ]
        geom = geom_ref[...].astype(jnp.float32)
        wide[chans : chans + 3, 0:hidden] = geom[3:6]
        row = lax.broadcasted_iota(jnp.int32, (LANES, LANES), 0)
        value = lax.broadcasted_iota(jnp.int32, (LANES, LANES), 1) - hidden
        pair = member // 2
        half = (value >= chans).astype(jnp.int32)
        take = (value >= 0) & (value < 2 * chans)
        take = take & (row == (2 * pair + half) * width + value - half * chans)
        table_w[...] = jnp.where(take, 1.0, wide[...]).astype(jnp.bfloat16)

        square[...] = jnp.zeros((LANES, LANES), jnp.float32)
        square[0:hidden, 0:hidden] = 0.5 * hidden_ref[...].astype(jnp.float32)
        hidden_w[...] = square[...].T.astype(jnp.bfloat16)

        square[...] = jnp.zeros((LANES, LANES), jnp.float32)
        square[0:hidden, 0:channels] = 0.5 * out_ref[...].astype(jnp.float32)
        square[hidden : hidden + 1, 0:channels] = three_ref[...]
        square[...] = square[...].T
        spread[...] = jnp.zeros((LANES, LANES), jnp.float32)
        spread[hidden : hidden + 2 * chans, :] = square[pl.ds(2 * pair * chans, 2 * chans), :]
        square[...] = spread[...].T
        out_w[...] = jnp.where(row < hidden, square[...], 0.0).astype(jnp.bfloat16)
        vec_ref[...] = jnp.zeros((8, LANES), jnp.float32)
        vec_ref[0:1, 0:hidden] = two_ref[...]
        vec_ref[1:2, :] = square[hidden : hidden + 1, :]

        ids = first_id + lax.broadcasted_iota(jnp.int32, (nodes + 8, 1), 0)
        along_x = ((ids % GX).astype(jnp.float32) + 0.5) / GX
        along_y = ((ids // GX % GY).astype(jnp.float32) + 0.5) / GY
        along_z = ((ids // (GX * GY)).astype(jnp.float32) + 0.5) / depth
        term = geom[0:1] * along_x + geom[1:2] * along_y + geom[2:3] * along_z + one_ref[...]
        node_pre[...] = jnp.zeros((nodes + 8, LANES), jnp.float32)
        node_pre[:, 0:hidden] = term

    out = pl.pallas_call(
        kernel,
        out_shape=(
            jax.ShapeDtypeStruct((tall, slots), jnp.int32),
            jax.ShapeDtypeStruct((16, LANES), jnp.int32),
            jax.ShapeDtypeStruct((listed, LANES), jnp.int32),
            jax.ShapeDtypeStruct((nodes, slots), jnp.float32),
            jax.ShapeDtypeStruct((LANES, LANES), jnp.bfloat16),
            jax.ShapeDtypeStruct((LANES, LANES), jnp.bfloat16),
            jax.ShapeDtypeStruct((LANES, LANES), jnp.bfloat16),
            jax.ShapeDtypeStruct((nodes + 8, LANES), jnp.float32),
            jax.ShapeDtypeStruct((8, LANES), jnp.float32),
        ),
        in_specs=[HBM] * len(given),
        out_specs=(VMEM,) * 9,
        scratch_shapes=[pltpu.SMEM(neighbour_count.shape, jnp.int32)]
        + [pltpu.VMEM(array.shape, array.dtype) for array in given[1:]]
        + [
            pltpu.VMEM((LANES, LANES), jnp.float32),
            pltpu.VMEM((LANES, LANES), jnp.float32),
            pltpu.VMEM((LANES, LANES), jnp.float32),
            pltpu.SemaphoreType.DMA((len(given),)),
        ],
        name="prepare",
    )(*given)
    return out[:2], out[2], out[3:]


def select_points(blocks, coords, send_rows, send_count):
    groups = len(blocks)
    chans, points = blocks[0].shape
    width = LANES // groups
    send = send_rows.shape[0] * LANES
    unroll = 16

    def kernel(*refs):
        block_refs = refs[:groups]
        coords_ref, rows_ref, count_ref = refs[groups : groups + 3]
        own_ref, sent_ref, stack, table, picked = refs[groups + 3 :]
        member = lax.axis_index("chan")
        side = 1 - member % ZD
        for step in range(groups):
            base = pl.multiple_of((member ^ step) * width, width)
            empty = jnp.zeros((width - chans, points), jnp.bfloat16)
            stack[pl.ds(base, width), :] = jnp.concatenate([block_refs[step][...], empty], axis=0)
        stack[chans : chans + 3, :] = coords_ref[...]
        stack[chans + 3 : chans + 4, :] = jnp.ones((1, points), jnp.bfloat16)
        own = stack[...].T
        own_ref[...] = own
        table[...] = own.astype(jnp.float32)

        for base in range(0, send, unroll):
            rows = [
                table[pl.ds(rows_ref[at // LANES, at % LANES], 1), :] for at in range(base, base + unroll)
            ]
            for j in range(unroll):
                picked[base + j : base + j + 1, :] = rows[j]
        slot = lax.broadcasted_iota(jnp.int32, (send, LANES), 0)
        sent_ref[...] = jnp.where(slot < count_ref[side, 0], picked[...], 0.0).astype(jnp.bfloat16)

    return pl.pallas_call(
        kernel,
        out_shape=(
            jax.ShapeDtypeStruct((points, LANES), jnp.bfloat16),
            jax.ShapeDtypeStruct((send, LANES), jnp.bfloat16),
        ),
        in_specs=[VMEM] * (groups + 1) + [SMEM] * 2,
        out_specs=(VMEM, VMEM),
        scratch_shapes=[
            pltpu.VMEM((LANES, points), jnp.bfloat16),
            pltpu.VMEM((points, LANES), jnp.float32),
            pltpu.VMEM((send, LANES), jnp.float32),
        ],
        compiler_params=pltpu.CompilerParams(vmem_limit_bytes=12 << 20),
        name="select_points",
    )(*blocks, coords, send_rows, send_count)


def encode(own, other, plan, weights, chans, hidden):
    rows, spots = plan
    halo, table_weight, hidden_weight, out_weight, node_part, vectors = weights
    points = own.shape[0]
    send = other.shape[0]
    nodes = node_part.shape[0] - 8
    slots = rows.shape[1]
    total_rows = points + send
    pairs = BLOCK * CHUNK
    lines = pairs // slots

    def kernel(
        own_ref, other_ref, rows_ref, spots_ref, halo_ref, table_w, hidden_w, out_w, node_pre,
        vec_ref, keep_ref, give_ref, table, picked, names_a, names_b, spot_ref, acc, turned,
        arrived,
    ):
        parity = 1 - lax.axis_index("chan") % ZD

        def fetch(block, names, which):
            source = rows_ref.at[pl.ds(pl.multiple_of(block * lines, lines), lines), :]
            return pltpu.make_async_copy(source, names, arrived.at[which])

        fetch(0, names_a, 0).start()
        fetch(1, names_b, 1).start()
        of_blocks = pltpu.make_async_copy(spots_ref, spot_ref, arrived.at[2])
        of_blocks.start()

        def fill(source, start, count):
            step = 256
            for at in range(0, count, step):
                both = jnp.dot(source[pl.ds(at, step), :], table_w[...], preferred_element_type=jnp.float32)
                table[start + at : start + at + step, :] = both.astype(jnp.bfloat16).astype(jnp.float32)

        fill(own_ref, 0, points)
        fill(other_ref, points, send)
        table[total_rows : total_rows + 8, :] = jnp.zeros((8, LANES), jnp.float32)
        acc[...] = jnp.zeros((nodes + 8, 8, LANES), jnp.float32)

        def one_block(block, names):
            for base in range(0, pairs, CHUNK):
                got = [
                    table[pl.ds(names[at // slots, at % slots], 1), :] for at in range(base, base + CHUNK)
                ]
                for j in range(CHUNK):
                    picked[base + j : base + j + 1, :] = got[j]
            step = 8
            for group in range(BLOCK // step):
                base = group * step * CHUNK
                here = [spot_ref[block, group * step + i] for i in range(step)]
                offset = jnp.concatenate(
                    [jnp.broadcast_to(node_pre[pl.ds(spot, 1), :], (CHUNK, LANES)) for spot in here],
                    axis=0,
                )
                row = picked[base : base + step * CHUNK, :]
                first = gelu_doubled(row + offset).astype(jnp.bfloat16)
                second = jnp.dot(first, hidden_w[...], preferred_element_type=jnp.float32)
                second = gelu_doubled(second + vec_ref[0:1]).astype(jnp.bfloat16)
                kappa = jnp.dot(second, out_w[...], preferred_element_type=jnp.float32) + vec_ref[1:2]
                product = kappa * row
                for i, spot in enumerate(here):
                    part = product[i * CHUNK : i * CHUNK + 8]
                    for j in range(8, CHUNK, 8):
                        part = part + product[i * CHUNK + j : i * CHUNK + j + 8]
                    acc[spot] = acc[spot] + part

        def one_step(index, carry):
            block = 2 * index
            fetch(block, names_a, 0).wait()
            one_block(block, names_a)
            fetch(block + 2, names_a, 0).start()
            fetch(block + 1, names_b, 1).wait()

            @pl.when(block + 1 < spot_ref[spots.shape[0] - 1, 0])
            def _():
                one_block(block + 1, names_b)

            fetch(block + 3, names_b, 1).start()
            return carry

        of_blocks.wait()
        blocks = spot_ref[spots.shape[0] - 1, 0]
        lax.fori_loop(0, (blocks + 1) // 2, one_step, 0)
        fetch(0, names_a, 0).wait()
        fetch(1, names_b, 1).wait()
        live = jnp.sum(other_ref[:, chans + 3 : chans + 4].astype(jnp.float32), axis=0, keepdims=True)
        used = jnp.where(halo_ref[...] < live, 1.0, 0.0)
        used = jnp.sum(used, axis=1, keepdims=True)
        means = (jnp.sum(acc[0:nodes], axis=1) / used).T
        low = jnp.where(parity == 1, means, 0.0)
        turned[...] = jnp.concatenate([low, means - low], axis=1)
        first = turned[hidden : hidden + chans, :]
        second = turned[hidden + chans : hidden + 2 * chans, :]
        keep_ref[...] = jnp.where(parity == 1, first, second)
        give_ref[...] = jnp.where(parity == 1, second, first)

    piece = jax.ShapeDtypeStruct((chans, ZD * nodes), jnp.float32)
    return pl.pallas_call(
        kernel,
        out_shape=(piece, piece),
        in_specs=[VMEM] * 10,
        out_specs=(VMEM, VMEM),
        scratch_shapes=[
            pltpu.VMEM((total_rows + 8, LANES), jnp.float32),
            pltpu.VMEM((pairs, LANES), jnp.float32),
            pltpu.SMEM((lines, slots), jnp.int32),
            pltpu.SMEM((lines, slots), jnp.int32),
            pltpu.SMEM(spots.shape, jnp.int32),
            pltpu.VMEM((nodes + 8, 8, LANES), jnp.float32),
            pltpu.VMEM((LANES, ZD * nodes), jnp.float32),
            pltpu.SemaphoreType.DMA((3,)),
        ],
        compiler_params=pltpu.CompilerParams(vmem_limit_bytes=16 << 20),
        name="encode",
    )(
        own, other, rows, spots, halo, table_weight, hidden_weight, out_weight, node_part, vectors
    )


def shards(
    features,
    coords,
    send_rows,
    send_count,
    neighbours,
    neighbour_count,
    geom_weight,
    feat_weight,
    bias_one,
    hidden_weight,
    bias_two,
    out_weight,
    bias_three,
):
    groups = lax.axis_size("chan")
    slabs = lax.axis_size("slab")
    chans, points = features.shape

    blocks = [features]
    for step in range(1, groups):
        blocks.append(lax.ppermute(features, "chan", [(i, i ^ step) for i in range(groups)]))

    plan, sent_rows, weights = prepare(
        neighbours, neighbour_count, geom_weight, feat_weight, bias_one, hidden_weight, bias_two,
        out_weight, bias_three, groups, points, send_rows, ZD * slabs,
    )
    own, sent = select_points(blocks, coords, sent_rows, send_count)
    moves = []
    for slab in range(slabs):
        for who in range(groups):
            target = slab + 1 if who % 2 == 0 else slab - 1
            if 0 <= target < slabs:
                moves.append((slab * groups + who, target * groups + who))
    other = lax.ppermute(sent, ("slab", "chan"), moves)
    keep, give = encode(own, other, plan, weights, chans, hidden_weight.shape[0])
    return keep + lax.ppermute(give, "chan", [(i, i ^ 1) for i in range(groups)])


def solution(mesh):
    placed = (
        P("chan", "slab"),
        P(None, "slab"),
        P(None, "slab"),
        P(None, "slab"),
        P("slab", None),
        P("slab"),
        P(),
        P(),
        P(),
        P(),
        P(),
        P(),
        P(),
    )
    return jax.shard_map(
        shards, mesh=mesh, in_specs=placed, out_specs=P("chan", "slab"), check_vma=False
    )
```

```python
import jax
import jax.numpy as jnp
from jax import lax
from jax.experimental import pallas as pl
from jax.experimental.pallas import tpu as pltpu
from jax.sharding import PartitionSpec as P


ZD = 2
GX = 16
GY = 4
LANES = 128
CHUNK = 16
BLOCK = 64
CONSTANT = 16.0
GELU_ONE = 0.7978845608028654
GELU_CUBE = 0.044715 * GELU_ONE

SMEM = pl.BlockSpec(memory_space=pltpu.SMEM)
VMEM = pl.BlockSpec(memory_space=pltpu.VMEM)
HBM = pl.BlockSpec(memory_space=pltpu.MemorySpace.HBM)


def gelu_doubled(x):
    inner = x * (GELU_ONE + GELU_CUBE * (x * x))
    return x * (1.0 + jnp.tanh(inner))


def prepare(
    neighbours, neighbour_count, geom_weight, feat_weight, bias_one, hidden_weight, bias_two,
    out_weight, bias_three, groups, points, send_rows, depth,
):
    per_slab, slots = neighbours.shape
    send = send_rows.shape[1]
    hidden, channels = feat_weight.shape
    chans = channels // groups
    width = LANES // groups
    nodes = per_slab // ZD
    per_node = slots // CHUNK
    most = nodes * per_node
    nothing = 2 * (points + send)
    extra = slice(hidden, hidden + 3)

    def parts(value):
        high = value.astype(jnp.bfloat16).astype(jnp.float32)
        mid = (value - high).astype(jnp.bfloat16).astype(jnp.float32)
        low = (value - high - mid).astype(jnp.bfloat16).astype(jnp.float32)
        return jnp.concatenate([high, mid, low], axis=0) * (1.0 / CONSTANT)

    given = (
        neighbour_count, neighbours, geom_weight.T, feat_weight, bias_one[None], hidden_weight,
        bias_two[None], out_weight.T, bias_three[None],
    )
    tall = most * CHUNK // slots + 3 * BLOCK * CHUNK // slots

    def kernel(*refs):
        rows_ref, spot_ref, table_w, hidden_w, out_w, node_pre = refs[len(given) :][:6]
        held = refs[len(given) + 6 :][: len(given)]
        wide, square, spread, arrived = refs[2 * len(given) + 6 :]
        copies = [
            pltpu.make_async_copy(source, target, arrived.at[at])
            for at, (source, target) in enumerate(zip(refs, held))
        ]
        for copy in copies:
            copy.start()
        for copy in copies:
            copy.wait()
        count_ref, nbr_ref, geom_ref, feat_ref, one_ref, hidden_ref, two_ref, out_ref, three_ref = held
        member = lax.axis_index("chan")
        start = (member % ZD) * nodes
        first_id = lax.axis_index("slab") * per_slab + start
        lane = lax.broadcasted_iota(jnp.int32, (1, LANES), 1)

        slot = lax.broadcasted_iota(jnp.int32, (1, slots), 1)
        rows_ref[...] = jnp.full((tall, slots), nothing, jnp.int32)
        together = 8

        chunk = BLOCK * lax.broadcasted_iota(jnp.int32, (8, LANES), 0)
        chunk = chunk + lax.broadcasted_iota(jnp.int32, (8, LANES), 1)

        def some_nodes(step, carry):
            at, node_of = carry
            first = step * together
            counts = [count_ref[start + first + i] for i in range(together)]
            spots = []
            for i in range(together):
                spots.append(at)
                at = at + (counts[i] + CHUNK - 1) // CHUNK
            turned = []
            for i in range(together):
                row = nbr_ref[pl.ds(start + first + i, 1), :]
                row = jnp.where(row >= points + send, row - send, row)
                row = jnp.where(slot < counts[i], 2 * row, nothing)
                turned.append(pltpu.roll(row, (spots[i] % per_node) * CHUNK, 1))
            for i in range(together):
                line = spots[i] // per_node
                kept = slot < (spots[i] % per_node) * CHUNK
                rows_ref[pl.ds(line, 1), :] = jnp.where(kept, rows_ref[pl.ds(line, 1), :], turned[i])
                rows_ref[pl.ds(line + 1, 1), :] = turned[i]
            for end in spots[1:] + [at]:
                node_of = node_of + (chunk >= end).astype(jnp.int32)
            return at, node_of

        none = jnp.zeros((8, LANES), jnp.int32)
        used, node_of = lax.fori_loop(0, nodes // together, some_nodes, (jnp.int32(0), none))
        spot_ref[0:8, :] = node_of
        spot_ref[8:16, :] = none + (used + BLOCK - 1) // BLOCK

        square[...] = jnp.zeros((LANES, LANES), jnp.float32)
        square[0:hidden, 0:channels] = feat_ref[...].astype(jnp.float32)
        square[...] = square[...].T
        wide[...] = jnp.zeros((LANES, 2 * LANES), jnp.float32)
        for block in range(groups):
            wide[block * width : block * width + chans, 0:LANES] = square[
                block * chans : (block + 1) * chans, :
            ]
        geom = geom_ref[...].astype(jnp.float32)
        wide[chans : chans + 3, 0:hidden] = geom[3:6]
        row = lax.broadcasted_iota(jnp.int32, (LANES, LANES), 0)
        col = lax.broadcasted_iota(jnp.int32, (LANES, LANES), 1)
        pair = member // 2
        take = ((row == pair * 2 * width + col) & (col < 2 * width)) | (
            (row == chans + 3) & (col == LANES - 1)
        )
        wide[:, LANES:] = take.astype(jnp.float32)
        table_w[...] = wide[...].astype(jnp.bfloat16)

        square[...] = jnp.zeros((LANES, LANES), jnp.float32)
        square[0:hidden, 0:hidden] = 0.5 * hidden_ref[...].astype(jnp.float32)
        square[...] = square[...].T
        square[extra, 0:hidden] = parts(two_ref[...])
        ones = (lane >= hidden) & (lane < hidden + 3)
        square[hidden : hidden + 1, hidden:] = jnp.where(ones, 0.5, 0.0)[:, hidden:]
        hidden_w[...] = square[...].astype(jnp.bfloat16)

        square[...] = jnp.zeros((LANES, LANES), jnp.float32)
        square[0:hidden, 0:channels] = 0.5 * out_ref[...].astype(jnp.float32)
        square[extra, 0:channels] = parts(three_ref[...])
        square[...] = square[...].T
        spread[...] = jnp.zeros((LANES, LANES), jnp.float32)
        for half in range(2):
            spread[half * width : half * width + chans, :] = square[
                pl.ds((2 * pair + half) * chans, chans), :
            ]
        spread[LANES - 1 :, :] = jnp.where(lane == hidden, 1.0 / CONSTANT, 0.0)
        out_w[...] = spread[...].T.astype(jnp.bfloat16)

        ids = first_id + lax.broadcasted_iota(jnp.int32, (nodes + 8, 1), 0)
        along_x = ((ids % GX).astype(jnp.float32) + 0.5) / GX
        along_y = ((ids // GX % GY).astype(jnp.float32) + 0.5) / GY
        along_z = ((ids // (GX * GY)).astype(jnp.float32) + 0.5) / depth
        term = geom[0:1] * along_x + geom[1:2] * along_y + geom[2:3] * along_z + one_ref[...]
        node_pre[...] = jnp.broadcast_to(jnp.where(ones, 0.5 * CONSTANT, 0.0), (nodes + 8, LANES))
        node_pre[:, 0:hidden] = term

    out = pl.pallas_call(
        kernel,
        out_shape=(
            jax.ShapeDtypeStruct((tall, slots), jnp.int32),
            jax.ShapeDtypeStruct((16, LANES), jnp.int32),
            jax.ShapeDtypeStruct((LANES, 2 * LANES), jnp.bfloat16),
            jax.ShapeDtypeStruct((LANES, LANES), jnp.bfloat16),
            jax.ShapeDtypeStruct((LANES, LANES), jnp.bfloat16),
            jax.ShapeDtypeStruct((nodes + 8, LANES), jnp.float32),
        ),
        in_specs=[HBM] * len(given),
        out_specs=(VMEM,) * 6,
        scratch_shapes=[pltpu.SMEM(neighbour_count.shape, jnp.int32)]
        + [pltpu.VMEM(array.shape, array.dtype) for array in given[1:]]
        + [
            pltpu.VMEM((LANES, 2 * LANES), jnp.float32),
            pltpu.VMEM((LANES, LANES), jnp.float32),
            pltpu.VMEM((LANES, LANES), jnp.float32),
            pltpu.SemaphoreType.DMA((len(given),)),
        ],
        name="prepare",
    )(*given)
    return out[:2], out[2:]


def select_points(blocks, coords, send_rows, send_count):
    groups = len(blocks)
    chans, points = blocks[0].shape
    width = LANES // groups
    send = send_rows.shape[1]
    unroll = 16

    def kernel(*refs):
        block_refs = refs[:groups]
        coords_ref, lists_ref, count_ref = refs[groups : groups + 3]
        own_ref, sent_ref, stack, table, picked, lines, rows_ref, arrived = refs[groups + 3 :]
        member = lax.axis_index("chan")
        side = 1 - member % ZD
        chosen = lists_ref[pl.ds(side, 1), :]
        for line in range(send // LANES):
            lines[line : line + 1, :] = chosen[:, line * LANES : (line + 1) * LANES]
        listed = pltpu.make_async_copy(lines, rows_ref, arrived)
        listed.start()
        for step in range(groups):
            base = pl.multiple_of((member ^ step) * width, width)
            empty = jnp.zeros((width - chans, points), jnp.bfloat16)
            stack[pl.ds(base, width), :] = jnp.concatenate([block_refs[step][...], empty], axis=0)
        stack[chans : chans + 3, :] = coords_ref[...]
        stack[chans + 3 : chans + 4, :] = jnp.ones((1, points), jnp.bfloat16)
        own = stack[...].T
        own_ref[...] = own
        table[...] = own.astype(jnp.float32)

        listed.wait()
        for base in range(0, send, unroll):
            rows = [
                table[pl.ds(rows_ref[at // LANES, at % LANES], 1), :] for at in range(base, base + unroll)
            ]
            for j in range(unroll):
                picked[base + j : base + j + 1, :] = rows[j]
        slot = lax.broadcasted_iota(jnp.int32, (send, LANES), 0)
        sent_ref[...] = jnp.where(slot < count_ref[0, side], picked[...], 0.0).astype(jnp.bfloat16)

    return pl.pallas_call(
        kernel,
        out_shape=(
            jax.ShapeDtypeStruct((points, LANES), jnp.bfloat16),
            jax.ShapeDtypeStruct((send, LANES), jnp.bfloat16),
        ),
        in_specs=[VMEM] * (groups + 2) + [SMEM],
        out_specs=(VMEM, VMEM),
        scratch_shapes=[
            pltpu.VMEM((LANES, points), jnp.bfloat16),
            pltpu.VMEM((points, LANES), jnp.float32),
            pltpu.VMEM((send, LANES), jnp.float32),
            pltpu.VMEM((send // LANES, LANES), jnp.int32),
            pltpu.SMEM((send // LANES, LANES), jnp.int32),
            pltpu.SemaphoreType.DMA,
        ],
        compiler_params=pltpu.CompilerParams(vmem_limit_bytes=12 << 20),
        name="select_points",
    )(*blocks, coords, send_rows, send_count)


def encode(own, other, plan, weights, chans, width):
    rows, spots = plan
    table_weight, hidden_weight, out_weight, node_part = weights
    points = own.shape[0]
    send = other.shape[0]
    nodes = node_part.shape[0] - 8
    slots = rows.shape[1]
    total_rows = points + send
    pairs = BLOCK * CHUNK
    lines = pairs // slots

    def kernel(
        own_ref, other_ref, rows_ref, spots_ref, table_w, hidden_w, out_w, node_pre,
        keep_ref, give_ref, table, picked, names_a, names_b, spot_ref, acc, turned,
        arrived,
    ):
        parity = 1 - lax.axis_index("chan") % ZD

        def fetch(block, names, which):
            source = rows_ref.at[pl.ds(pl.multiple_of(block * lines, lines), lines), :]
            return pltpu.make_async_copy(source, names, arrived.at[which])

        fetch(0, names_a, 0).start()
        fetch(1, names_b, 1).start()
        of_blocks = pltpu.make_async_copy(spots_ref, spot_ref, arrived.at[2])
        of_blocks.start()

        def fill(source, start, count):
            step = 256
            for at in range(0, count, step):
                both = jnp.dot(source[pl.ds(at, step), :], table_w[...], preferred_element_type=jnp.float32)
                pre = both[:, :LANES].astype(jnp.bfloat16).astype(jnp.float32)
                table[pl.ds(2 * (start + at), step, stride=2), :] = pre
                table[pl.ds(2 * (start + at) + 1, step, stride=2), :] = both[:, LANES:]

        fill(own_ref, 0, points)
        fill(other_ref, points, send)
        table[pl.ds(2 * total_rows, 8), :] = jnp.zeros((8, LANES), jnp.float32)
        acc[...] = jnp.zeros((nodes + 8, 8, LANES), jnp.float32)

        def one_block(block, names):
            for base in range(0, pairs, CHUNK):
                got = [
                    table[pl.ds(names[at // slots, at % slots], 2), :] for at in range(base, base + CHUNK)
                ]
                for j in range(CHUNK):
                    picked[2 * (base + j) : 2 * (base + j) + 2, :] = got[j]
            step = 8
            for group in range(BLOCK // step):
                base = group * step * CHUNK
                here = [spot_ref[block, group * step + i] for i in range(step)]
                offset = jnp.concatenate(
                    [jnp.broadcast_to(node_pre[pl.ds(spot, 1), :], (CHUNK, LANES)) for spot in here],
                    axis=0,
                )
                pre = picked[pl.ds(2 * base, step * CHUNK, stride=2), :]
                val = picked[pl.ds(2 * base + 1, step * CHUNK, stride=2), :]
                first = gelu_doubled(pre + offset).astype(jnp.bfloat16)
                second = jnp.dot(first, hidden_w[...], preferred_element_type=jnp.float32)
                second = gelu_doubled(second).astype(jnp.bfloat16)
                kappa = jnp.dot(second, out_w[...], preferred_element_type=jnp.float32)
                product = kappa * val
                for i, spot in enumerate(here):
                    part = product[i * CHUNK : i * CHUNK + 8]
                    for j in range(8, CHUNK, 8):
                        part = part + product[i * CHUNK + j : i * CHUNK + j + 8]
                    acc[spot] = acc[spot] + part

        def one_step(index, carry):
            block = 2 * index
            fetch(block, names_a, 0).wait()
            one_block(block, names_a)
            fetch(block + 2, names_a, 0).start()
            fetch(block + 1, names_b, 1).wait()

            @pl.when(block + 1 < spot_ref[spots.shape[0] - 1, 0])
            def _():
                one_block(block + 1, names_b)

            fetch(block + 3, names_b, 1).start()
            return carry

        of_blocks.wait()
        blocks = spot_ref[spots.shape[0] - 1, 0]
        lax.fori_loop(0, (blocks + 1) // 2, one_step, 0)
        fetch(0, names_a, 0).wait()
        fetch(1, names_b, 1).wait()
        sums = jnp.sum(acc[0:nodes], axis=1)
        means = (sums / sums[:, LANES - 1 :]).T
        low = jnp.where(parity == 1, means, 0.0)
        turned[...] = jnp.concatenate([low, means - low], axis=1)
        mine = pl.multiple_of((1 - parity) * width, width)
        theirs = pl.multiple_of(parity * width, width)
        keep_ref[...] = turned[pl.ds(mine, chans), :]
        give_ref[...] = turned[pl.ds(theirs, chans), :]

    piece = jax.ShapeDtypeStruct((chans, ZD * nodes), jnp.float32)
    return pl.pallas_call(
        kernel,
        out_shape=(piece, piece),
        in_specs=[VMEM] * 8,
        out_specs=(VMEM, VMEM),
        scratch_shapes=[
            pltpu.VMEM((2 * total_rows + 8, LANES), jnp.float32),
            pltpu.VMEM((2 * pairs, LANES), jnp.float32),
            pltpu.SMEM((lines, slots), jnp.int32),
            pltpu.SMEM((lines, slots), jnp.int32),
            pltpu.SMEM(spots.shape, jnp.int32),
            pltpu.VMEM((nodes + 8, 8, LANES), jnp.float32),
            pltpu.VMEM((LANES, ZD * nodes), jnp.float32),
            pltpu.SemaphoreType.DMA((3,)),
        ],
        compiler_params=pltpu.CompilerParams(vmem_limit_bytes=16 << 20),
        name="encode",
    )(own, other, rows, spots, table_weight, hidden_weight, out_weight, node_part)


def shards(
    features,
    coords,
    send_rows,
    send_count,
    neighbours,
    neighbour_count,
    geom_weight,
    feat_weight,
    bias_one,
    hidden_weight,
    bias_two,
    out_weight,
    bias_three,
):
    groups = lax.axis_size("chan")
    slabs = lax.axis_size("slab")
    chans, points = features.shape
    width = LANES // groups

    blocks = [features]
    for step in range(1, groups):
        blocks.append(lax.ppermute(features, "chan", [(i, i ^ step) for i in range(groups)]))

    plan, weights = prepare(
        neighbours, neighbour_count, geom_weight, feat_weight, bias_one, hidden_weight, bias_two,
        out_weight, bias_three, groups, points, send_rows, ZD * slabs,
    )

    own, sent = select_points(blocks, coords, send_rows, send_count.T)
    moves = []
    for slab in range(slabs):
        for who in range(groups):
            target = slab + 1 if who % 2 == 0 else slab - 1
            if 0 <= target < slabs:
                moves.append((slab * groups + who, target * groups + who))
    other = lax.ppermute(sent, ("slab", "chan"), moves)
    keep, give = encode(own, other, plan, weights, chans, width)
    return keep + lax.ppermute(give, "chan", [(i, i ^ 1) for i in range(groups)])


def solution(mesh):
    placed = (
        P("chan", "slab"),
        P(None, "slab"),
        P(None, "slab"),
        P(None, "slab"),
        P("slab", None),
        P("slab"),
        P(),
        P(),
        P(),
        P(),
        P(),
        P(),
        P(),
    )
    return jax.shard_map(
        shards, mesh=mesh, in_specs=placed, out_specs=P("chan", "slab"), check_vma=False
    )
```
